128 devices in a mesh: shard: 32 (over z, x, core), replica: 4 (over y).
Axes of the slice: x: 4, y: 4, z: 4, core: 2. Of those that a mesh axis runs over, the one named last changes fastest.
Arguments:
- samples: bfloat16 [8192, 480, 128], P(('shard', 'replica')), may hold values from -6 to 6
- counts: int32 [8192], P(('shard', 'replica')), may hold values from 1 to 480
- buckets: int32 [8192, 480], P(('shard', 'replica')), may hold values from 0 to 127
- block_series: int32 [8192], P(('shard', 'replica')), may hold values from 0 to 255, as said below
- owner_map: int32 [256], replicated, may hold values from 0 to 255
Outputs:
- cold_stats: float32 [32, 4, 128, 4, 8, 128], P('shard', 'replica')
- sketches: float32 [256, 128, 128], P(('shard', 'replica'))
- live_rows: float32 [256], P(('shard', 'replica'))
The draws below stay inside these ranges and needn't reach their ends.
Inputs may be any that keep to these rules, and one draw needn't show every extreme that they name: `block_series`: owner_map is a permutation of 0 to 255. With owner = owner_map[series] // 8, the 64 blocks of one device name at most 4 blocks of any one owner, and in every draw some owner gets exactly 4 blocks from every device.
All inputs are finite; a program needn't handle non-finite values.
Results may differ from the reference program's by a relative error of at most 0.0003.
Values may be sent and summed in bfloat16 or wider, within the bound.
A program may use at most 192 MiB of HBM per device.

```python
import jax
import jax.numpy as jnp
from jax import lax

LANES = 128
BINS = 128
MINUTES = 8
BLK_DEV = 64
SAMPLES = 480
BLOCKS = 8192
SER_OWN = 8
SERIES = 256
CAP = 4
HEAVY = 4
N_SHARD = 32
N_REPLICA = 4


def routing(key):
    owner_map = jax.random.permutation(jax.random.fold_in(key, 11), SERIES).astype(jnp.int32)
    inverse = jnp.argsort(owner_map).astype(jnp.int32)
    order = jax.random.permutation(jax.random.fold_in(key, 12), N_SHARD)
    heavy = jnp.zeros((N_SHARD,), jnp.int32).at[order[:HEAVY]].set(1)
    devices = N_SHARD * N_REPLICA
    width = N_SHARD * CAP
    candidate = jnp.arange(width, dtype=jnp.int32) // CAP
    noise = jax.random.randint(jax.random.fold_in(key, 13), (devices, width), 0, 1 << 20)
    score = (noise + heavy[candidate][None, :] * (1 << 21)) * width + jnp.arange(width, dtype=jnp.int32)[None, :]
    _, picked = lax.top_k(score, BLK_DEV)
    owners = candidate[picked]
    shuffle = jax.random.randint(jax.random.fold_in(key, 14), (devices, BLK_DEV), 0, 1 << 20) * BLK_DEV
    shuffle = shuffle + jnp.arange(BLK_DEV, dtype=jnp.int32)[None, :]
    owners = jnp.take_along_axis(owners, jnp.argsort(shuffle, axis=1), axis=1)
    local = jax.random.randint(jax.random.fold_in(key, 15), (devices, BLK_DEV), 0, SER_OWN)
    series = inverse[(owners * SER_OWN + local).reshape(-1)]
    return (owner_map, series.astype(jnp.int32))


def draw_owner_map(key, part):
    return routing(key)[0]


def draw_block_series(key, part):
    return routing(key)[1]


def with_ends(result, stream_key, smallest, high):
    shape = result.shape
    index_at = [jax.random.randint(jax.random.fold_in(stream_key, axis), (), 0, shape[axis]) for axis in range(len(shape))]
    result = result.at[tuple(index_at)].set(smallest)
    longest = shape.index(max(shape))
    index_at[longest] = (index_at[longest] + 1) % shape[longest]
    return result.at[tuple(index_at)].set(high)


def block_levels(stream_key, extent, cuts, low, largest):
    factor_of = 1.0
    for dim, shards_of in cuts:
        heights = jax.random.uniform(jax.random.fold_in(jax.random.fold_in(stream_key, 6), dim), (shards_of,), jnp.float32, low / len(cuts), largest / len(cuts))
        factor_of = factor_of * jnp.repeat(jnp.exp(heights), extent[dim] // shards_of).reshape((-1,) + (1,) * (len(extent) - 1 - dim))
    return factor_of


def bell_draw(stream_key, dims, scale, bound, pieces=(), kind=jnp.bfloat16):
    array = jax.random.normal(stream_key, dims, jnp.float32) * scale
    if len(pieces) > 0:
        array = block_levels(stream_key, dims, pieces, -0.22, 0.18) * array
    return jnp.clip(array, min=-bound, max=bound).astype(kind)


def setup_inputs(seed: int = 0) -> dict:
    key_list = jax.random.split(jax.random.key(seed), 6)
    return {
        "samples": bell_draw(key_list[0], (BLOCKS, SAMPLES, LANES), 1.0, 6.0, ((0, 128),)),
        "counts": with_ends(jax.random.randint(key_list[1], (BLOCKS,), 1, SAMPLES + 1), jax.random.fold_in(key_list[1], 1), 1, SAMPLES).astype(jnp.int32),
        "buckets": with_ends(jax.random.randint(key_list[2], (BLOCKS, SAMPLES), 0, BINS), jax.random.fold_in(key_list[2], 1), 0, BINS - 1).astype(jnp.int32),
        "block_series": draw_block_series(jax.random.fold_in(key_list[5], 71), 0),
        "owner_map": draw_owner_map(jax.random.fold_in(key_list[5], 71), 0),
    }


def minute_stats(values, counts):
    blocks, samples, lanes = values.shape
    minutes = samples // 60
    steps = jnp.arange(samples, dtype=jnp.int32)
    live = (steps[None, :] < counts[:, None]).reshape(blocks, minutes, 60, 1)
    data = values.astype(jnp.float32).reshape(blocks, minutes, 60, lanes)
    count = jnp.sum(jnp.where(live, jnp.float32(1.0), jnp.float32(0.0)), axis=2)
    count = jnp.broadcast_to(count, (blocks, minutes, lanes))
    total = jnp.sum(jnp.where(live, data, jnp.float32(0.0)), axis=2)
    lowest = jnp.min(jnp.where(live, data, jnp.inf), axis=2)
    highest = jnp.max(jnp.where(live, data, -jnp.inf), axis=2)
    filled = count > 0
    lowest = jnp.where(filled, lowest, jnp.float32(0.0))
    highest = jnp.where(filled, highest, jnp.float32(0.0))
    return jnp.stack([lowest, highest, total, count], axis=1)


def reference(samples, counts, buckets, block_series, owner_map):
    groups = N_SHARD * N_REPLICA
    position = owner_map[block_series].astype(jnp.int32)
    owner = position // SER_OWN
    grouped = owner.reshape(N_SHARD, N_REPLICA, BLK_DEV)
    index = jnp.arange(BLK_DEV, dtype=jnp.int32)
    same = (grouped[..., :, None] == grouped[..., None, :]) & (index[None, :] < index[:, None])
    rank = jnp.sum(same.astype(jnp.int32), axis=-1)
    source = jnp.broadcast_to(jnp.arange(N_SHARD, dtype=jnp.int32)[:, None, None], rank.shape)
    replica = jnp.broadcast_to(jnp.arange(N_REPLICA, dtype=jnp.int32)[None, :, None], rank.shape)
    values_g = samples.reshape(groups, BLK_DEV, SAMPLES, LANES)
    counts_g = counts.reshape(groups, BLK_DEV)
    stats = lax.map(lambda item: minute_stats(item[0], item[1]), (values_g, counts_g))
    stats = stats.reshape(N_SHARD, N_REPLICA, BLK_DEV, 4, MINUTES, LANES)
    cold = jnp.zeros((N_SHARD, N_REPLICA, N_SHARD * CAP, 4, MINUTES, LANES), jnp.float32)
    cold = cold.at[grouped, replica, source * CAP + rank].set(stats)
    steps = jnp.arange(SAMPLES, dtype=jnp.int32)
    marks_g = buckets.reshape(groups, BLK_DEV, SAMPLES)
    places_g = position.reshape(groups, BLK_DEV)

    def accumulate(carry, item):
        values, marks, live_count, places = item
        live = steps[None, :] < live_count[:, None]
        ids = jnp.where(live, places[:, None] * BINS + marks, SERIES * BINS).astype(jnp.int32)
        data = values.astype(jnp.float32).reshape(-1, LANES)
        return carry + jax.ops.segment_sum(data, ids.reshape(-1), num_segments=SERIES * BINS + 1), None

    start = jnp.zeros((SERIES * BINS + 1, LANES), jnp.float32)
    total, _ = lax.scan(accumulate, start, (values_g, marks_g, counts_g, places_g))
    sketches = total[:SERIES * BINS].reshape(SERIES, BINS, LANES)
    live_rows = jax.ops.segment_sum(counts.astype(jnp.float32), position, num_segments=SERIES)
    return cold, sketches, live_rows
```

```python
import functools

import jax
import jax.numpy as jnp
import numpy as np
from jax import lax
from jax.experimental import pallas as pl
from jax.experimental.pallas import tpu as pltpu
from jax.sharding import PartitionSpec as P

BINS = 128
LANES = 128
SAMPLES = 480
BLK = 64
SHARDS = 32
REPLICAS = 4
CAP = 4
DIMS = (("x", 0), ("z", 0), ("y", 0), ("x", 1), ("z", 1), ("y", 1))
ORDERS = tuple(tuple((p + s) % 6 for s in range(6)) for p in range(6))
ROWS = (16, 16, 32, 16, 16, 32)
STARTS = tuple(sum(ROWS[:p]) for p in range(6))
GRAY = {(0, 0): 0, (0, 1): 1, (1, 1): 2, (1, 0): 3}


def part_positions():
    table = np.zeros((6, 128), np.int32)
    for p, order in enumerate(ORDERS):
        for i in range(128):
            bits = {DIMS[d]: (i >> (6 - s)) & 1 for s, d in enumerate(order)}
            x, y, z = (GRAY[(bits[(a, 1)], bits[(a, 0)])] for a in "xyz")
            table[p, i] = (z * 4 + x) * 16 + y * 2 + (i & 1)
    return table


def local_kernel(idx_ref, samples_ref, marks_ref, table_ref, stats_ref, *, step):
    base = pl.program_id(0) * step
    rows = lax.broadcasted_iota(jnp.int32, (1, SAMPLES), 1)
    bins = lax.broadcasted_iota(jnp.int32, (BINS, SAMPLES), 0)
    first_row = lax.broadcasted_iota(jnp.int32, (16, SAMPLES), 0) * 60
    sub = lax.broadcasted_iota(jnp.int32, (8, LANES), 0)
    for j in range(step):
        b = base + j
        slot, fresh, place, count = idx_ref[0, b], idx_ref[1, b], idx_ref[2, b], idx_ref[3, b]
        x = samples_ref[j]
        live = rows < count
        marks = jnp.where(live, marks_ref[pl.ds(b, 1), :], -1)
        hot = jnp.where(bins == marks, 1.0, 0.0).astype(jnp.bfloat16)
        at = jnp.where(live, rows, -1)
        minute = jnp.where((at >= first_row) & (at < first_row + 60), 1.0, 0.0).astype(jnp.bfloat16)
        both = jnp.dot(jnp.concatenate([hot, minute], axis=0), x, preferred_element_type=jnp.float32)
        old = table_ref[slot]
        table_ref[slot] = jnp.where(fresh == 1, 0.0, old) + both[:BINS]
        total = both[BINS : BINS + 8]
        high = total.astype(jnp.bfloat16)
        low = (total - high.astype(jnp.float32)).astype(jnp.bfloat16)
        least = jnp.zeros((8, LANES), jnp.float32)
        most = jnp.zeros((8, LANES), jnp.float32)
        for q in range(4):
            lo = [None, None]
            hi = [None, None]
            for v in range(15):
                at_row = 120 * q + 8 * v
                val = x[at_row : at_row + 8].astype(jnp.float32)
                ok = sub < count - at_row
                small = jnp.where(ok, val, jnp.inf)
                large = jnp.where(ok, val, -jnp.inf)
                for h in (0, 1):
                    if (h == 0 and v > 7) or (h == 1 and v < 7):
                        continue
                    s, g = small, large
                    if v == 7:
                        mine = (sub < 4) if h == 0 else (sub >= 4)
                        s, g = jnp.where(mine, s, jnp.inf), jnp.where(mine, g, -jnp.inf)
                    lo[h] = s if lo[h] is None else jnp.minimum(lo[h], s)
                    hi[h] = g if hi[h] is None else jnp.maximum(hi[h], g)
            for h in (0, 1):
                m = 2 * q + h
                least = jnp.where(sub == m, jnp.min(lo[h], axis=0, keepdims=True), least)
                most = jnp.where(sub == m, jnp.max(hi[h], axis=0, keepdims=True), most)
        stats_ref[place] = jnp.concatenate(
            [least.astype(jnp.bfloat16), most.astype(jnp.bfloat16), high, low], axis=0
        )


def local_call(idx, samples, marks):
    step = 4
    return pl.pallas_call(
        functools.partial(local_kernel, step=step),
        grid=(BLK // step,),
        in_specs=[
            pl.BlockSpec(memory_space=pltpu.SMEM),
            pl.BlockSpec((step, SAMPLES, LANES), lambda i: (i, 0, 0)),
            pl.BlockSpec((BLK, SAMPLES), lambda i: (0, 0)),
        ],
        out_specs=[
            pl.BlockSpec((SHARDS * CAP, BINS, LANES), lambda i: (0, 0, 0)),
            pl.BlockSpec((SHARDS * CAP, 32, LANES), lambda i: (0, 0, 0)),
        ],
        out_shape=[
            jax.ShapeDtypeStruct((SHARDS * CAP, BINS, LANES), jnp.float32),
            jax.ShapeDtypeStruct((SHARDS * CAP, 32, LANES), jnp.bfloat16),
        ],
        compiler_params=pltpu.CompilerParams(vmem_limit_bytes=56 * 2**20),
        name="local_stats",
    )(idx, samples, marks)


def exchange_kernel(
    own_idx, prt_idx, table, stats, meta, live,
    sk_out, stats_out, meta_out, live_out,
    *scratch,
):
    own, prt, acc, got = scratch[0:6], scratch[6:12], scratch[12:18], scratch[18:24]
    mine_st, mine_meta, rows_in, lbuf, lgot = scratch[24:29]
    own_sem, d2d_send, d2d_recv, cube_send, cube_recv, st_send, st_recv, l_send, l_recv, loc_sem = scratch[29:39]
    shard = lax.axis_index("shard")
    y = lax.axis_index("replica")
    core = lax.rem(shard, 2)
    x = lax.rem(lax.div(shard, 2), 4)
    z = lax.div(shard, 8)
    where_at = {"x": x, "y": y, "z": z}

    def other(dim):
        axis, bit = dim
        v = where_at[axis]
        high = lax.div(v, 2)
        if bit == 0:
            mine = lax.rem(v + high, 2)
            w = v + 1 - 2 * lax.rem(v, 2)
        else:
            mine = high
            w = 3 - v
        if axis == "x":
            return {"shard": shard + (w - v) * 2, "replica": y}, mine
        if axis == "z":
            return {"shard": shard + (w - v) * 8, "replica": y}, mine
        return {"shard": shard, "replica": w}, mine

    across = [other(d) for d in DIMS]
    partner = {"shard": shard + 1 - 2 * core, "replica": y}

    barrier = pltpu.get_barrier_semaphore()

    def greet(d, _):
        pl.semaphore_signal(barrier, inc=1, device_id={"shard": lax.rem(shard + d, SHARDS), "replica": y})
        return 0

    lax.fori_loop(1, SHARDS, greet, 0)
    for d in (2, 5):
        pl.semaphore_signal(barrier, inc=1, device_id=across[d][0])
    own_copies = []
    for p in range(6):
        rows = pl.ds(STARTS[p], ROWS[p])
        c = pltpu.make_async_copy(table.at[core, :, rows], own[p].at[pl.ds(0, BLK)], own_sem.at[p])
        c.start()
        own_copies.append(c)
    st_in = pltpu.make_async_copy(stats.at[shard], mine_st, loc_sem.at[0])
    st_in.start()
    meta_in = pltpu.make_async_copy(meta.at[shard], mine_meta, loc_sem.at[1])
    meta_in.start()
    live_in = pltpu.make_async_copy(live, rows_in, loc_sem.at[2])
    live_in.start()
    for p in range(6):
        own[p][BLK] = jnp.zeros((ROWS[p], LANES), jnp.float32)
        prt[p][BLK] = jnp.zeros((ROWS[p], LANES), jnp.float32)
    pl.semaphore_wait(barrier, SHARDS + 1)

    def d2d(p):
        rows = pl.ds(STARTS[p], ROWS[p])
        return pltpu.make_async_remote_copy(
            table.at[1 - core, :, rows], prt[p].at[pl.ds(0, BLK)], d2d_send.at[p], d2d_recv.at[p], device_id=partner,
        )

    parts = (2, 5, 0, 1, 3, 4)
    d2d_copies = {p: d2d(p) for p in parts}
    for p in parts:
        d2d_copies[p].start()

    def st_copy(d, dst_shard, src_slot):
        return pltpu.make_async_remote_copy(
            stats.at[dst_shard], stats_out.at[src_slot], st_send.at[0, d], st_recv.at[0, d],
            device_id={"shard": dst_shard, "replica": y},
        )

    def meta_copy(d, dst_shard, src_slot):
        return pltpu.make_async_remote_copy(
            meta.at[dst_shard], meta_out.at[src_slot], st_send.at[1, d], st_recv.at[1, d],
            device_id={"shard": dst_shard, "replica": y},
        )

    def send_stats(d, _):
        to = lax.rem(shard + d, SHARDS)
        st_copy(d, to, shard).start()
        meta_copy(d, to, shard).start()
        return 0

    lax.fori_loop(1, SHARDS, send_stats, 0)
    st_in.wait()
    st_back = pltpu.make_async_copy(mine_st, stats_out.at[shard], loc_sem.at[3])
    st_back.start()
    meta_in.wait()
    meta_back = pltpu.make_async_copy(mine_meta, meta_out.at[shard], loc_sem.at[4])
    meta_back.start()
    live_in.wait()

    def live_copy(s, src, device):
        return pltpu.make_async_remote_copy(src, lgot.at[s], l_send.at[s], l_recv.at[s], device_id=device)

    live_copies = [live_copy(0, rows_in.at[1 - core], partner)]
    live_copies[0].start()

    bases = [[None] * 7 for _ in range(6)]
    copies = [[None] * 6 for _ in range(6)]

    def densify(p, lo):
        def body(i, _):
            for u in range(8):
                e = lo + i * 8 + u
                acc[p][e] = own[p][own_idx[p * 128 + e]] + prt[p][prt_idx[p * 128 + e]]
            return 0

        lax.fori_loop(0, 8, body, 0)

    def add_in(p, at, lo, n):
        unroll = min(n, 8)

        def body(i, _):
            for u in range(unroll):
                e = i * unroll + u
                acc[p][at + e] = acc[p][at + e] + got[p][lo + e]
            return 0

        lax.fori_loop(0, n // unroll, body, 0)

    def send(p, s):
        device, bit = across[ORDERS[p][s]]
        half = 64 >> s
        base = bases[p][s]
        c = pltpu.make_async_remote_copy(
            acc[p].at[pl.ds(base + (1 - bit) * half, half)],
            got[p].at[pl.ds(128 - (128 >> s), half)],
            cube_send.at[p, s], cube_recv.at[p, s], device_id=device,
        )
        c.start()
        copies[p][s] = c
        bases[p][s + 1] = base + bit * half

    for p in parts:
        own_copies[p].wait()
        d2d_copies[p].wait_recv()
        bases[p][0] = 0
        bit = across[ORDERS[p][0]][1]
        densify(p, (1 - bit) * 64)
        send(p, 0)
        densify(p, bit * 64)

    live_copies[0].wait_recv()
    lbuf[0] = rows_in[core] + lgot[0]
    for s in range(1, 7):
        live_copies.append(live_copy(s, lbuf.at[s - 1], across[ORDERS[0][s - 1]][0]))
        live_copies[s].start()
        for p in parts:
            copies[p][s - 1].wait_recv()
            half = 64 >> (s - 1)
            lo = 128 - (128 >> (s - 1))
            base = bases[p][s]
            if s < 6:
                quarter = half // 2
                bit = across[ORDERS[p][s]][1]
                add_in(p, base + (1 - bit) * quarter, lo + (1 - bit) * quarter, quarter)
                send(p, s)
                add_in(p, base + bit * quarter, lo + bit * quarter, quarter)
            else:
                for k in range(2):
                    sk_out[k, STARTS[p] : STARTS[p] + ROWS[p], :] = acc[p][base + k] + got[p][lo + k]
        live_copies[s].wait_recv()
        lbuf[s] = lbuf[s - 1] + lgot[s]
    live_out[...] = lbuf[6]

    def wait_stats(d, _):
        came = lax.rem(shard - d + SHARDS, SHARDS)
        st_copy(d, shard, came).wait_recv()
        meta_copy(d, shard, came).wait_recv()
        return 0

    lax.fori_loop(1, SHARDS, wait_stats, 0)

    def wait_sends(d, _):
        to = lax.rem(shard + d, SHARDS)
        st_copy(d, to, shard).wait_send()
        meta_copy(d, to, shard).wait_send()
        return 0

    lax.fori_loop(1, SHARDS, wait_sends, 0)
    st_back.wait()
    meta_back.wait()
    for c in live_copies:
        c.wait_send()
    for p in range(6):
        d2d_copies[p].wait_send()
        for s in range(6):
            copies[p][s].wait_send()


def exchange_call(own_idx, prt_idx, table, stats, meta, live):
    any_ = pl.BlockSpec(memory_space=pl.ANY)
    vmem = pl.BlockSpec(memory_space=pltpu.VMEM)
    smem = pl.BlockSpec(memory_space=pltpu.SMEM)
    f32 = jnp.float32
    scratch = (
        [pltpu.VMEM((BLK + 1, r, LANES), f32) for r in ROWS]
        + [pltpu.VMEM((BLK + 1, r, LANES), f32) for r in ROWS]
        + [pltpu.VMEM((128, r, LANES), f32) for r in ROWS]
        + [pltpu.VMEM((126, r, LANES), f32) for r in ROWS]
        + [
            pltpu.VMEM((CAP, 32, LANES), jnp.bfloat16),
            pltpu.VMEM((1, LANES), f32),
            pltpu.VMEM((2, 1, LANES), f32),
            pltpu.VMEM((7, 1, LANES), f32),
            pltpu.VMEM((7, 1, LANES), f32),
        ]
        + [
            pltpu.SemaphoreType.DMA((6,)),
            pltpu.SemaphoreType.DMA((6,)),
            pltpu.SemaphoreType.DMA((6,)),
            pltpu.SemaphoreType.DMA((6, 6)),
            pltpu.SemaphoreType.DMA((6, 6)),
            pltpu.SemaphoreType.DMA((2, SHARDS)),
            pltpu.SemaphoreType.DMA((2, SHARDS)),
            pltpu.SemaphoreType.DMA((7,)),
            pltpu.SemaphoreType.DMA((7,)),
            pltpu.SemaphoreType.DMA((5,)),
        ]
    )
    return pl.pallas_call(
        exchange_kernel,
        in_specs=[smem, smem, any_, any_, any_, any_],
        out_specs=[vmem, any_, any_, vmem],
        out_shape=[
            jax.ShapeDtypeStruct((2, BINS, LANES), f32),
            jax.ShapeDtypeStruct((SHARDS, CAP, 32, LANES), jnp.bfloat16),
            jax.ShapeDtypeStruct((SHARDS, 1, LANES), f32),
            jax.ShapeDtypeStruct((1, LANES), f32),
        ],
        scratch_shapes=scratch,
        compiler_params=pltpu.CompilerParams(
            collective_id=0, has_side_effects=True, vmem_limit_bytes=56 * 2**20
        ),
        name="exchange",
    )(own_idx, prt_idx, table, stats, meta, live)


def finish_kernel(counts, stats_ref, sk_ref, live_ref, cold_ref, sk_out, live_out, *, step):
    i = pl.program_id(0)
    minute = lax.broadcasted_iota(jnp.int32, (8, LANES), 0).astype(jnp.float32) * 60.0
    for j in range(step):
        at = i * step + j
        n = counts[lax.div(at, CAP), 0, lax.rem(at, CAP)]
        count = jnp.clip(n - minute, 0.0, 60.0)
        filled = count > 0
        st = stats_ref[j].astype(jnp.float32)
        cold_ref[j, 0] = jnp.where(filled, st[0:8], 0.0)
        cold_ref[j, 1] = jnp.where(filled, st[8:16], 0.0)
        cold_ref[j, 2] = jnp.where(filled, st[16:24] + st[24:32], 0.0)
        cold_ref[j, 3] = count

    @pl.when(i == 0)
    def _():
        sk_out[...] = sk_ref[...]
        at = lax.div(lax.axis_index("shard"), 2) * 8 + lax.axis_index("replica") * 2
        lane = lax.broadcasted_iota(jnp.int32, (1, LANES), 1)
        for k in range(2):
            live_out[k] = jnp.sum(jnp.where(lane == at + k, live_ref[...], 0.0))


def finish_call(counts, stats, sketches, live):
    step = 16
    return pl.pallas_call(
        functools.partial(finish_kernel, step=step),
        grid=(SHARDS * CAP // step,),
        in_specs=[
            pl.BlockSpec(memory_space=pltpu.SMEM),
            pl.BlockSpec((step, 32, LANES), lambda i: (i, 0, 0)),
            pl.BlockSpec((2, BINS, LANES), lambda i: (0, 0, 0)),
            pl.BlockSpec((1, LANES), lambda i: (0, 0)),
        ],
        out_specs=[
            pl.BlockSpec((step, 4, 8, LANES), lambda i: (i, 0, 0, 0)),
            pl.BlockSpec((2, BINS, LANES), lambda i: (0, 0, 0)),
            pl.BlockSpec(memory_space=pltpu.SMEM),
        ],
        out_shape=[
            jax.ShapeDtypeStruct((SHARDS * CAP, 4, 8, LANES), jnp.float32),
            jax.ShapeDtypeStruct((2, BINS, LANES), jnp.float32),
            jax.ShapeDtypeStruct((2,), jnp.float32),
        ],
        name="finish",
    )(counts, stats, sketches, live)


def positions_of(block_series, owner_map):
    series = jnp.arange(owner_map.shape[0], dtype=jnp.int32)
    return jnp.sum(jnp.where(block_series[:, None] == series[None, :], owner_map[None, :], 0), axis=1)


def slots_of(position):
    owner = position // 8
    index = jnp.arange(BLK, dtype=jnp.int32)
    earlier = index[None, :] < index[:, None]
    rank = jnp.sum(((owner[:, None] == owner[None, :]) & earlier).astype(jnp.int32), axis=1)
    return owner, rank, (owner // 2) * CAP + rank


def body(samples, counts, buckets, block_series, owner_map):
    core = lax.axis_index("shard") % 2
    swap = [(i, i ^ 1) for i in range(SHARDS)]
    their_series = lax.ppermute(block_series, "shard", swap)
    position = positions_of(block_series, owner_map)
    owner, rank, half_slot = slots_of(position)
    same = position[:, None] == position[None, :]
    first_slot = jnp.min(jnp.where(same, half_slot[None, :], 2 * BLK), axis=1)
    fresh = (first_slot == half_slot).astype(jnp.int32)
    place = owner * CAP + rank
    idx = jnp.stack([(owner % 2) * BLK + first_slot, fresh, place, counts])
    table, stats = local_call(idx, samples, buckets)

    target = jnp.asarray(part_positions().reshape(-1)) + core * 8

    def entries(pos, slot):
        hit = target[:, None] == pos[None, :]
        return jnp.min(jnp.where(hit, slot[None, :], BLK), axis=1)

    own_idx = entries(position, half_slot)
    their_position = positions_of(their_series, owner_map)
    prt_idx = entries(their_position, slots_of(their_position)[2])
    rows = counts.astype(jnp.float32)
    lane = np.arange(128)
    live_at = jnp.asarray(np.stack([(lane // 8) * 16 + r * 8 + lane % 8 for r in (0, 1)]).astype(np.int32))
    live = jnp.sum(jnp.where(live_at[:, :, None] == position[None, None, :], rows[None, None, :], 0.0), axis=2)
    at = np.where(lane[None, :] < CAP, np.arange(SHARDS)[:, None] * CAP + lane[None, :], -1).astype(np.int32)
    meta = jnp.sum(jnp.where(jnp.asarray(at)[:, :, None] == place[None, None, :], rows[None, None, :], 0.0), axis=2)
    sk, st, got_counts, got_live = exchange_call(
        own_idx, prt_idx,
        table.reshape(2, BLK, BINS, LANES), stats.reshape(SHARDS, CAP, 32, LANES),
        meta.reshape(SHARDS, 1, LANES), live.reshape(2, 1, LANES),
    )
    cold, sketches, live_rows = finish_call(got_counts, st.reshape(SHARDS * CAP, 32, LANES), sk, got_live)
    return cold.reshape(1, 1, SHARDS * CAP, 4, 8, LANES), sketches, live_rows


def solution(mesh):
    return jax.shard_map(
        body,
        mesh=mesh,
        in_specs=(
            P(("shard", "replica"), None, None),
            P(("shard", "replica")),
            P(("shard", "replica"), None),
            P(("shard", "replica")),
            P(),
        ),
        out_specs=(
            P("shard", "replica", None, None, None, None),
            P(("shard", "replica"), None, None),
            P(("shard", "replica")),
        ),
        check_vma=False,
    )
```

```python
import functools

import jax
import jax.numpy as jnp
import numpy as np
from jax import lax
from jax.experimental import pallas as pl
from jax.experimental.pallas import tpu as pltpu
from jax.sharding import PartitionSpec as P

BINS = 128
LANES = 128
SAMPLES = 480
BLK = 64
SHARDS = 32
REPLICAS = 4
CAP = 4
DIMS = (("x", 0), ("z", 0), ("y", 0), ("x", 1), ("z", 1), ("y", 1))
ORDERS = (
    (5, 2, 4, 0, 3, 1), (5, 4, 1, 2, 0, 3), (2, 5, 1, 3, 4, 0), (0, 1, 4, 3, 5, 2),
    (2, 0, 3, 4, 1, 5), (3, 2, 5, 4, 1, 0), (4, 3, 0, 5, 2, 1), (1, 5, 2, 0, 3, 4),
)
PARTS = len(ORDERS)
ROWS = BINS // PARTS
LEVELS = 32766.0
TINY = 1e-33
GRAY = {(0, 0): 0, (0, 1): 1, (1, 1): 2, (1, 0): 3}


def part_positions():
    table = np.zeros((PARTS, 128), np.int32)
    for p, order in enumerate(ORDERS):
        for i in range(128):
            bits = {DIMS[d]: (i >> (6 - s)) & 1 for s, d in enumerate(order)}
            x, y, z = (GRAY[(bits[(a, 1)], bits[(a, 0)])] for a in "xyz")
            table[p, i] = (z * 4 + x) * 16 + y * 2 + (i & 1)
    return table


def local_kernel(idx_ref, samples_ref, marks_ref, table_ref, stats_ref, *, step):
    base = pl.program_id(0) * step
    rows = lax.broadcasted_iota(jnp.int32, (1, SAMPLES), 1)
    bins = lax.broadcasted_iota(jnp.int32, (BINS, SAMPLES), 0)
    first_row = lax.broadcasted_iota(jnp.int32, (16, SAMPLES), 0) * 60
    sub = lax.broadcasted_iota(jnp.int32, (8, LANES), 0)
    for j in range(step):
        b = base + j
        slot, fresh, place, count = idx_ref[0, b], idx_ref[1, b], idx_ref[2, b], idx_ref[3, b]
        x = samples_ref[j]
        live = rows < count
        marks = jnp.where(live, marks_ref[pl.ds(b, 1), :], -1)
        hot = jnp.where(bins == marks, 1.0, 0.0).astype(jnp.bfloat16)
        at = jnp.where(live, rows, -1)
        minute = jnp.where((at >= first_row) & (at < first_row + 60), 1.0, 0.0).astype(jnp.bfloat16)
        both = jnp.dot(jnp.concatenate([hot, minute], axis=0), x, preferred_element_type=jnp.float32)
        old = table_ref[slot]
        table_ref[slot] = jnp.where(fresh == 1, 0.0, old) + both[:BINS]
        total = both[BINS : BINS + 8]
        high = total.astype(jnp.bfloat16)
        low = (total - high.astype(jnp.float32)).astype(jnp.bfloat16)
        least = jnp.zeros((8, LANES), jnp.float32)
        most = jnp.zeros((8, LANES), jnp.float32)
        for q in range(4):
            lo = [None, None]
            hi = [None, None]
            for v in range(15):
                at_row = 120 * q + 8 * v
                val = x[at_row : at_row + 8].astype(jnp.float32)
                ok = sub < count - at_row
                small = jnp.where(ok, val, jnp.inf)
                large = jnp.where(ok, val, -jnp.inf)
                for h in (0, 1):
                    if (h == 0 and v > 7) or (h == 1 and v < 7):
                        continue
                    s, g = small, large
                    if v == 7:
                        mine = (sub < 4) if h == 0 else (sub >= 4)
                        s, g = jnp.where(mine, s, jnp.inf), jnp.where(mine, g, -jnp.inf)
                    lo[h] = s if lo[h] is None else jnp.minimum(lo[h], s)
                    hi[h] = g if hi[h] is None else jnp.maximum(hi[h], g)
            for h in (0, 1):
                m = 2 * q + h
                least = jnp.where(sub == m, jnp.min(lo[h], axis=0, keepdims=True), least)
                most = jnp.where(sub == m, jnp.max(hi[h], axis=0, keepdims=True), most)
        stats_ref[place] = jnp.concatenate(
            [least.astype(jnp.bfloat16), most.astype(jnp.bfloat16), high, low], axis=0
        )


def local_call(idx, samples, marks):
    step = 4
    return pl.pallas_call(
        functools.partial(local_kernel, step=step),
        grid=(BLK // step,),
        in_specs=[
            pl.BlockSpec(memory_space=pltpu.SMEM),
            pl.BlockSpec((step, SAMPLES, LANES), lambda i: (i, 0, 0)),
            pl.BlockSpec((BLK, SAMPLES), lambda i: (0, 0)),
        ],
        out_specs=[
            pl.BlockSpec((SHARDS * CAP, BINS, LANES), lambda i: (0, 0, 0)),
            pl.BlockSpec((SHARDS * CAP, 32, LANES), lambda i: (0, 0, 0)),
        ],
        out_shape=[
            jax.ShapeDtypeStruct((SHARDS * CAP, BINS, LANES), jnp.float32),
            jax.ShapeDtypeStruct((SHARDS * CAP, 32, LANES), jnp.bfloat16),
        ],
        compiler_params=pltpu.CompilerParams(vmem_limit_bytes=56 * 2**20),
        name="local_stats",
    )(idx, samples, marks)


def exchange_kernel(
    own_idx, prt_idx, table, stats, meta, live,
    sk_out, stats_out, meta_out, live_out,
    *scratch,
):
    own, prt, acc, out, outs, got, gots = (scratch[PARTS * i : PARTS * (i + 1)] for i in range(7))
    mine_st, mine_meta, rows_in, lbuf, lgot = scratch[7 * PARTS : 7 * PARTS + 5]
    (own_sem, d2d_send, d2d_recv, cube_send, cube_recv, st_send, st_recv, l_send, l_recv, loc_sem) = scratch[7 * PARTS + 5 :]
    shard = lax.axis_index("shard")
    y = lax.axis_index("replica")
    core = lax.rem(shard, 2)
    x = lax.rem(lax.div(shard, 2), 4)
    z = lax.div(shard, 8)
    where_at = {"x": x, "y": y, "z": z}

    def other(dim):
        axis, bit = dim
        v = where_at[axis]
        high = lax.div(v, 2)
        if bit == 0:
            mine = lax.rem(v + high, 2)
            w = v + 1 - 2 * lax.rem(v, 2)
        else:
            mine = high
            w = 3 - v
        if axis == "x":
            return {"shard": shard + (w - v) * 2, "replica": y}, mine
        if axis == "z":
            return {"shard": shard + (w - v) * 8, "replica": y}, mine
        return {"shard": shard, "replica": w}, mine

    across = [other(d) for d in DIMS]
    partner = {"shard": shard + 1 - 2 * core, "replica": y}

    barrier = pltpu.get_barrier_semaphore()

    def greet(d, _):
        pl.semaphore_signal(barrier, inc=1, device_id={"shard": lax.rem(shard + d, SHARDS), "replica": y})
        return 0

    lax.fori_loop(1, SHARDS, greet, 0)
    for d in (2, 5):
        pl.semaphore_signal(barrier, inc=1, device_id=across[d][0])
    own_copies = []
    for p in range(PARTS):
        rows = pl.ds(p * ROWS, ROWS)
        c = pltpu.make_async_copy(table.at[core, :, rows], own[p].at[pl.ds(0, BLK)], own_sem.at[p])
        c.start()
        own_copies.append(c)
    st_in = pltpu.make_async_copy(stats.at[shard], mine_st, loc_sem.at[0])
    st_in.start()
    meta_in = pltpu.make_async_copy(meta.at[shard], mine_meta, loc_sem.at[1])
    meta_in.start()
    live_in = pltpu.make_async_copy(live, rows_in, loc_sem.at[2])
    live_in.start()
    for p in range(PARTS):
        own[p][BLK] = jnp.zeros((ROWS, LANES), jnp.float32)
        prt[p][BLK] = jnp.zeros((ROWS, LANES), jnp.float32)
    pl.semaphore_wait(barrier, SHARDS + 1)

    def d2d(p):
        rows = pl.ds(p * ROWS, ROWS)
        return pltpu.make_async_remote_copy(
            table.at[1 - core, :, rows], prt[p].at[pl.ds(0, BLK)], d2d_send.at[p], d2d_recv.at[p], device_id=partner,
        )

    parts = tuple(range(PARTS))
    d2d_copies = {p: d2d(p) for p in parts}
    for p in parts:
        d2d_copies[p].start()

    def st_copy(d, dst_shard, src_slot):
        return pltpu.make_async_remote_copy(
            stats.at[dst_shard], stats_out.at[src_slot], st_send.at[0, d], st_recv.at[0, d],
            device_id={"shard": dst_shard, "replica": y},
        )

    def meta_copy(d, dst_shard, src_slot):
        return pltpu.make_async_remote_copy(
            meta.at[dst_shard], meta_out.at[src_slot], st_send.at[1, d], st_recv.at[1, d],
            device_id={"shard": dst_shard, "replica": y},
        )

    def send_stats(d, _):
        to = lax.rem(shard + d, SHARDS)
        st_copy(d, to, shard).start()
        meta_copy(d, to, shard).start()
        return 0

    lax.fori_loop(1, SHARDS, send_stats, 0)
    st_in.wait()
    st_back = pltpu.make_async_copy(mine_st, stats_out.at[shard], loc_sem.at[3])
    st_back.start()
    meta_in.wait()
    meta_back = pltpu.make_async_copy(mine_meta, meta_out.at[shard], loc_sem.at[4])
    meta_back.start()
    live_in.wait()

    def live_copy(s, src, device):
        return pltpu.make_async_remote_copy(src, lgot.at[s], l_send.at[s], l_recv.at[s], device_id=device)

    live_copies = [live_copy(0, rows_in.at[1 - core], partner)]
    live_copies[0].start()

    bases = [[None] * 7 for _ in parts]
    copies = [[None] * 6 for _ in parts]

    def encode(v):
        size = jnp.max(jnp.abs(v), axis=0, keepdims=True)
        gain = jnp.where(size > TINY, LEVELS / jnp.maximum(size, TINY), 0.0)
        code = (v * gain + 32768.5).astype(jnp.int32)
        return (code[:8] << 16) | code[8:], size

    def decode(word, size):
        unit = size * (1.0 / LEVELS)
        high = lax.shift_right_logical(word, 16).astype(jnp.float32)
        low = (word & 0xFFFF).astype(jnp.float32)
        return jnp.concatenate([(high - 32768.0) * unit, (low - 32768.0) * unit], axis=0)

    def each(n, fn):
        unroll = min(n, 8)

        def body(i, _):
            for u in range(unroll):
                fn(i * unroll + u)
            return 0

        lax.fori_loop(0, n // unroll, body, 0)

    def densify(p, lo, to=None):
        def one(i):
            e = lo + i
            v = own[p][own_idx[p * 128 + e]] + prt[p][prt_idx[p * 128 + e]]
            if to is None:
                acc[p][e] = v
            else:
                out[p][to + i], outs[p][to + i] = encode(v)

        each(64, one)

    def add_in(p, at, lo, n, to=None):
        def one(i):
            v = acc[p][at + i] + decode(got[p][lo + i], gots[p][lo + i])
            if to is None:
                acc[p][at + i] = v
            else:
                out[p][to + i], outs[p][to + i] = encode(v)

        each(n, one)

    def offset(s):
        return 128 - (128 >> s)

    def send(p, s):
        device, bit = across[ORDERS[p][s]]
        half = 64 >> s
        region = pl.ds(offset(s), half)
        both = []
        for k, (src, dst) in enumerate(((out, got), (outs, gots))):
            c = pltpu.make_async_remote_copy(
                src[p].at[region], dst[p].at[region], cube_send.at[k, p, s], cube_recv.at[k, p, s], device_id=device,
            )
            c.start()
            both.append(c)
        copies[p][s] = both
        bases[p][s + 1] = bases[p][s] + bit * half

    for p in parts:
        own_copies[p].wait()
        d2d_copies[p].wait_recv()
        bases[p][0] = 0
        bit = across[ORDERS[p][0]][1]
        densify(p, (1 - bit) * 64, 0)
        send(p, 0)
        densify(p, bit * 64)

    live_copies[0].wait_recv()
    lbuf[0] = rows_in[core] + lgot[0]
    for s in range(1, 7):
        live_copies.append(live_copy(s, lbuf.at[s - 1], across[ORDERS[0][s - 1]][0]))
        live_copies[s].start()
        for p in parts:
            for c in copies[p][s - 1]:
                c.wait_recv()
            half = 64 >> (s - 1)
            lo = offset(s - 1)
            base = bases[p][s]
            if s < 6:
                quarter = half // 2
                bit = across[ORDERS[p][s]][1]
                away = (1 - bit) * quarter
                add_in(p, base + away, lo + away, quarter, offset(s))
                send(p, s)
                add_in(p, base + bit * quarter, lo + bit * quarter, quarter)
            else:
                for k in range(2):
                    v = acc[p][base + k] + decode(got[p][lo + k], gots[p][lo + k])
                    sk_out[k, p * ROWS : (p + 1) * ROWS, :] = v
        live_copies[s].wait_recv()
        lbuf[s] = lbuf[s - 1] + lgot[s]
    live_out[...] = lbuf[6]

    def wait_stats(d, _):
        came = lax.rem(shard - d + SHARDS, SHARDS)
        st_copy(d, shard, came).wait_recv()
        meta_copy(d, shard, came).wait_recv()
        return 0

    lax.fori_loop(1, SHARDS, wait_stats, 0)

    def wait_sends(d, _):
        to = lax.rem(shard + d, SHARDS)
        st_copy(d, to, shard).wait_send()
        meta_copy(d, to, shard).wait_send()
        return 0

    lax.fori_loop(1, SHARDS, wait_sends, 0)
    st_back.wait()
    meta_back.wait()
    for c in live_copies:
        c.wait_send()
    for p in parts:
        d2d_copies[p].wait_send()
        for s in range(6):
            for c in copies[p][s]:
                c.wait_send()


def exchange_call(own_idx, prt_idx, table, stats, meta, live):
    any_ = pl.BlockSpec(memory_space=pl.ANY)
    vmem = pl.BlockSpec(memory_space=pltpu.VMEM)
    smem = pl.BlockSpec(memory_space=pltpu.SMEM)
    f32 = jnp.float32
    scratch = (
        [pltpu.VMEM((BLK + 1, ROWS, LANES), f32)] * (2 * PARTS)
        + [pltpu.VMEM((128, ROWS, LANES), f32)] * PARTS
        + [pltpu.VMEM((126, 8, LANES), jnp.int32)] * PARTS
        + [pltpu.VMEM((126, 1, LANES), f32)] * PARTS
        + [pltpu.VMEM((126, 8, LANES), jnp.int32)] * PARTS
        + [pltpu.VMEM((126, 1, LANES), f32)] * PARTS
        + [
            pltpu.VMEM((CAP, 32, LANES), jnp.bfloat16),
            pltpu.VMEM((1, LANES), f32),
            pltpu.VMEM((2, 1, LANES), f32),
            pltpu.VMEM((7, 1, LANES), f32),
            pltpu.VMEM((7, 1, LANES), f32),
        ]
        + [
            pltpu.SemaphoreType.DMA((PARTS,)),
            pltpu.SemaphoreType.DMA((PARTS,)),
            pltpu.SemaphoreType.DMA((PARTS,)),
            pltpu.SemaphoreType.DMA((2, PARTS, 6)),
            pltpu.SemaphoreType.DMA((2, PARTS, 6)),
            pltpu.SemaphoreType.DMA((2, SHARDS)),
            pltpu.SemaphoreType.DMA((2, SHARDS)),
            pltpu.SemaphoreType.DMA((7,)),
            pltpu.SemaphoreType.DMA((7,)),
            pltpu.SemaphoreType.DMA((5,)),
        ]
    )
    return pl.pallas_call(
        exchange_kernel,
        in_specs=[smem, smem, any_, any_, any_, any_],
        out_specs=[vmem, any_, any_, vmem],
        out_shape=[
            jax.ShapeDtypeStruct((2, BINS, LANES), f32),
            jax.ShapeDtypeStruct((SHARDS, CAP, 32, LANES), jnp.bfloat16),
            jax.ShapeDtypeStruct((SHARDS, 1, LANES), f32),
            jax.ShapeDtypeStruct((1, LANES), f32),
        ],
        scratch_shapes=scratch,
        compiler_params=pltpu.CompilerParams(
            collective_id=0, has_side_effects=True, vmem_limit_bytes=56 * 2**20
        ),
        name="exchange",
    )(own_idx, prt_idx, table, stats, meta, live)


def finish_kernel(counts, stats_ref, sk_ref, live_ref, cold_ref, sk_out, live_out, *, step):
    i = pl.program_id(0)
    minute = lax.broadcasted_iota(jnp.int32, (8, LANES), 0).astype(jnp.float32) * 60.0
    for j in range(step):
        at = i * step + j
        n = counts[lax.div(at, CAP), 0, lax.rem(at, CAP)]
        count = jnp.clip(n - minute, 0.0, 60.0)
        filled = count > 0
        st = stats_ref[j].astype(jnp.float32)
        cold_ref[j, 0] = jnp.where(filled, st[0:8], 0.0)
        cold_ref[j, 1] = jnp.where(filled, st[8:16], 0.0)
        cold_ref[j, 2] = jnp.where(filled, st[16:24] + st[24:32], 0.0)
        cold_ref[j, 3] = count

    @pl.when(i == 0)
    def _():
        sk_out[...] = sk_ref[...]
        at = lax.div(lax.axis_index("shard"), 2) * 8 + lax.axis_index("replica") * 2
        lane = lax.broadcasted_iota(jnp.int32, (1, LANES), 1)
        for k in range(2):
            live_out[k] = jnp.sum(jnp.where(lane == at + k, live_ref[...], 0.0))


def finish_call(counts, stats, sketches, live):
    step = 32
    return pl.pallas_call(
        functools.partial(finish_kernel, step=step),
        grid=(SHARDS * CAP // step,),
        in_specs=[
            pl.BlockSpec(memory_space=pltpu.SMEM),
            pl.BlockSpec((step, 32, LANES), lambda i: (i, 0, 0)),
            pl.BlockSpec((2, BINS, LANES), lambda i: (0, 0, 0)),
            pl.BlockSpec((1, LANES), lambda i: (0, 0)),
        ],
        out_specs=[
            pl.BlockSpec((step, 4, 8, LANES), lambda i: (i, 0, 0, 0)),
            pl.BlockSpec((2, BINS, LANES), lambda i: (0, 0, 0)),
            pl.BlockSpec(memory_space=pltpu.SMEM),
        ],
        out_shape=[
            jax.ShapeDtypeStruct((SHARDS * CAP, 4, 8, LANES), jnp.float32),
            jax.ShapeDtypeStruct((2, BINS, LANES), jnp.float32),
            jax.ShapeDtypeStruct((2,), jnp.float32),
        ],
        name="finish",
    )(counts, stats, sketches, live)


def positions_of(block_series, owner_map):
    series = jnp.arange(owner_map.shape[0], dtype=jnp.int32)
    return jnp.sum(jnp.where(block_series[:, None] == series[None, :], owner_map[None, :], 0), axis=1)


def slots_of(position):
    owner = position // 8
    index = jnp.arange(BLK, dtype=jnp.int32)
    earlier = index[None, :] < index[:, None]
    rank = jnp.sum(((owner[:, None] == owner[None, :]) & earlier).astype(jnp.int32), axis=1)
    return owner, rank, (owner // 2) * CAP + rank


def body(samples, counts, buckets, block_series, owner_map):
    core = lax.axis_index("shard") % 2
    swap = [(i, i ^ 1) for i in range(SHARDS)]
    their_series = lax.ppermute(block_series, "shard", swap)
    position = positions_of(block_series, owner_map)
    owner, rank, half_slot = slots_of(position)
    same = position[:, None] == position[None, :]
    first_slot = jnp.min(jnp.where(same, half_slot[None, :], 2 * BLK), axis=1)
    fresh = (first_slot == half_slot).astype(jnp.int32)
    place = owner * CAP + rank
    idx = jnp.stack([(owner % 2) * BLK + first_slot, fresh, place, counts])
    table, stats = local_call(idx, samples, buckets)

    target = jnp.asarray(part_positions().reshape(-1)) + core * 8

    def entries(pos, slot):
        hit = target[:, None] == pos[None, :]
        return jnp.min(jnp.where(hit, slot[None, :], BLK), axis=1)

    own_idx = entries(position, half_slot)
    their_position = positions_of(their_series, owner_map)
    prt_idx = entries(their_position, slots_of(their_position)[2])
    rows = counts.astype(jnp.float32)
    lane = np.arange(128)
    live_at = jnp.asarray(np.stack([(lane // 8) * 16 + r * 8 + lane % 8 for r in (0, 1)]).astype(np.int32))
    live = jnp.sum(jnp.where(live_at[:, :, None] == position[None, None, :], rows[None, None, :], 0.0), axis=2)
    at = np.where(lane[None, :] < CAP, np.arange(SHARDS)[:, None] * CAP + lane[None, :], -1).astype(np.int32)
    meta = jnp.sum(jnp.where(jnp.asarray(at)[:, :, None] == place[None, None, :], rows[None, None, :], 0.0), axis=2)
    sk, st, got_counts, got_live = exchange_call(
        own_idx, prt_idx,
        table.reshape(2, BLK, BINS, LANES), stats.reshape(SHARDS, CAP, 32, LANES),
        meta.reshape(SHARDS, 1, LANES), live.reshape(2, 1, LANES),
    )
    cold, sketches, live_rows = finish_call(got_counts, st.reshape(SHARDS * CAP, 32, LANES), sk, got_live)
    return cold.reshape(1, 1, SHARDS * CAP, 4, 8, LANES), sketches, live_rows


def solution(mesh):
    return jax.shard_map(
        body,
        mesh=mesh,
        in_specs=(
            P(("shard", "replica"), None, None),
            P(("shard", "replica")),
            P(("shard", "replica"), None),
            P(("shard", "replica")),
            P(),
        ),
        out_specs=(
            P("shard", "replica", None, None, None, None),
            P(("shard", "replica"), None, None),
            P(("shard", "replica")),
        ),
        check_vma=False,
    )
```

```python
import functools

import jax
import jax.numpy as jnp
import numpy as np
from jax import lax
from jax.experimental import pallas as pl
from jax.experimental.pallas import tpu as pltpu
from jax.sharding import PartitionSpec as P

BINS = 128
LANES = 128
SAMPLES = 480
BLK = 64
SHARDS = 32
REPLICAS = 4
CAP = 4
DIMS = (("x", 0), ("z", 0), ("y", 0), ("x", 1), ("z", 1), ("y", 1))
ORDERS = (
    (5, 2, 4, 0, 3, 1), (5, 4, 1, 2, 0, 3), (2, 5, 1, 3, 4, 0), (0, 1, 4, 3, 5, 2),
    (2, 0, 3, 4, 1, 5), (3, 2, 5, 4, 1, 0), (4, 3, 0, 5, 2, 1), (1, 5, 2, 0, 3, 4),
)
PARTS = len(ORDERS)
ROWS = BINS // PARTS
LEVELS = 32766.0
TINY = 1e-33
GRAY = {(0, 0): 0, (0, 1): 1, (1, 1): 2, (1, 0): 3}


def part_positions():
    table = np.zeros((PARTS, 128), np.int32)
    for p, order in enumerate(ORDERS):
        for i in range(128):
            bits = {DIMS[d]: (i >> (6 - s)) & 1 for s, d in enumerate(order)}
            x, y, z = (GRAY[(bits[(a, 1)], bits[(a, 0)])] for a in "xyz")
            table[p, i] = (z * 4 + x) * 16 + y * 2 + (i & 1)
    return table


def minute_extremes(x, count):
    sub16 = lax.broadcasted_iota(jnp.int16, (16, LANES), 0)
    sub = lax.broadcasted_iota(jnp.int32, (8, LANES), 0)
    least = jnp.zeros((8, LANES), jnp.float32)
    most = jnp.zeros((8, LANES), jnp.float32)
    inf = jnp.bfloat16(jnp.inf)
    for q in range(2):
        lo = [None] * 4
        hi = [None] * 4
        for v in range(15):
            at_row = 240 * q + 16 * v
            val = x[at_row : at_row + 16]
            ok = sub16 < jnp.full((16, LANES), jnp.clip(count - at_row, 0, 16), jnp.int32).astype(jnp.int16)
            small, large = jnp.where(ok, val, inf), jnp.where(ok, val, -inf)
            for h in range(4):
                a, b = 60 * h - 16 * v, 60 * h + 60 - 16 * v
                if b <= 0 or a >= 16:
                    continue
                s, g = small, large
                if a > 0:
                    s, g = jnp.where(sub16 >= a, s, inf), jnp.where(sub16 >= a, g, -inf)
                if b < 16:
                    s, g = jnp.where(sub16 < b, s, inf), jnp.where(sub16 < b, g, -inf)
                lo[h] = s if lo[h] is None else jnp.minimum(lo[h], s)
                hi[h] = g if hi[h] is None else jnp.maximum(hi[h], g)
        for h in range(4):
            m = 4 * q + h
            least = jnp.where(sub == m, jnp.min(lo[h].astype(jnp.float32), axis=0, keepdims=True), least)
            most = jnp.where(sub == m, jnp.max(hi[h].astype(jnp.float32), axis=0, keepdims=True), most)
    return least.astype(jnp.bfloat16), most.astype(jnp.bfloat16)


def iota(shape, dim):
    return lax.broadcasted_iota(jnp.int32, shape, dim).astype(jnp.float32)


def routing(series_row, map_row):
    sub, lane = iota((BLK, BLK), 0), iota((BLK, BLK), 1)
    eye = sub == lane

    def row(col):
        return jnp.sum(jnp.where(eye, col, 0.0), axis=0, keepdims=True)

    series = jnp.sum(jnp.where(eye, series_row, 0.0), axis=1, keepdims=True)
    pos = jnp.sum(jnp.where(iota((BLK, 256), 1) == series, map_row, 0.0), axis=1, keepdims=True)
    owner = jnp.floor(pos * 0.125)
    pos_r, owner_r = row(pos), row(owner)
    rank = jnp.sum(jnp.where((owner == owner_r) & (lane < sub), 1.0, 0.0), axis=1, keepdims=True)
    slot = jnp.floor(owner * 0.5) * CAP + rank
    return pos, owner, rank, slot, pos_r, owner_r, row(rank), row(slot)


def local_kernel(
    samples, marks_ref, counts_ref, series_ref, theirs_ref, map_ref, target_ref, live_at,
    table, stats, own_out, prt_out, meta_out, live_out,
    x_buf, t_buf, st_buf, idx_v, idx_ref, in_sem, t_sem, st_sem, idx_sem,
    *, step,
):
    steps = BLK // step
    for i in range(steps):
        part = pl.ds(i * step, step)
        pltpu.make_async_copy(samples.at[part], x_buf.at[part], in_sem.at[i]).start()

    map_row = map_ref[...].astype(jnp.float32)
    counts_row = counts_ref[...].astype(jnp.float32)
    pos, owner, rank, slot, pos_r, owner_r, rank_r, slot_r = routing(series_ref[...].astype(jnp.float32), map_row)
    sub, lane = iota((BLK, BLK), 0), iota((BLK, BLK), 1)
    same = pos == pos_r
    first = jnp.min(jnp.where(same, slot, 1000.0), axis=0, keepdims=True)
    later = jnp.max(jnp.where(same & (sub > lane), 1.0, 0.0), axis=0, keepdims=True)
    odd = owner_r - 2.0 * jnp.floor(owner_r * 0.5)
    rows = (
        odd * BLK + first,
        jnp.where(first == slot_r, 1.0, 0.0),
        owner_r * CAP + rank_r,
        counts_row,
        1.0 - later,
    )
    for r, value in enumerate(rows):
        idx_v[r : r + 1, 0:BLK] = value.astype(jnp.int32)
    idx_copy = pltpu.make_async_copy(idx_v, idx_ref, idx_sem)
    idx_copy.start()
    core = lax.rem(lax.axis_index("shard"), 2)
    their = routing(theirs_ref[...].astype(jnp.float32), map_row)
    for p in range(PARTS):
        want = (target_ref[p : p + 1, :] + core * 8).astype(jnp.float32)
        for out, (at, val) in ((own_out, (pos, slot)), (prt_out, (their[0], their[3]))):
            hit = jnp.min(jnp.where(at == want, val, float(BLK)), axis=0, keepdims=True)
            out[p : p + 1, :] = hit.astype(jnp.int32)
    counts_col = jnp.sum(jnp.where(sub == lane, counts_row, 0.0), axis=1, keepdims=True)
    for r in range(2):
        at = live_at[r : r + 1, :].astype(jnp.float32)
        live_out[r] = jnp.sum(jnp.where(pos == at, counts_col, 0.0), axis=0, keepdims=True)
    pick = jnp.where(iota((SHARDS, BLK), 0) == owner_r, 1.0, 0.0)
    put = jnp.where(iota((BLK, LANES), 1) == rank, counts_col, 0.0)
    meta = jnp.dot(pick, put, precision=lax.Precision.HIGHEST, preferred_element_type=jnp.float32)
    for o in range(SHARDS):
        meta_out[o] = meta[o : o + 1, :]
    idx_copy.wait()

    row_at = lax.broadcasted_iota(jnp.int32, (1, SAMPLES), 1)
    bins = lax.broadcasted_iota(jnp.int32, (BINS, SAMPLES), 0)
    first_row = lax.broadcasted_iota(jnp.int32, (16, SAMPLES), 0) * 60

    def t_copy(b):
        at = idx_ref[0, b]
        return pltpu.make_async_copy(t_buf.at[at], table.at[at], t_sem.at[b])

    def st_copy(b):
        return pltpu.make_async_copy(st_buf.at[b], stats.at[idx_ref[2, b]], st_sem.at[b])

    def chunk(i, _):
        part = pl.ds(i * step, step)
        pltpu.make_async_copy(samples.at[part], x_buf.at[part], in_sem.at[i]).wait()
        for j in range(step):
            b = i * step + j
            slot_b, fresh, count, last = idx_ref[0, b], idx_ref[1, b], idx_ref[3, b], idx_ref[4, b]
            x = x_buf[b]
            live = row_at < count
            marks = jnp.where(live, marks_ref[pl.ds(b, 1), :], -1)
            hot = jnp.where(bins == marks, 1.0, 0.0).astype(jnp.bfloat16)
            at = jnp.where(live, row_at, -1)
            minute = jnp.where((at >= first_row) & (at < first_row + 60), 1.0, 0.0).astype(jnp.bfloat16)
            both = jnp.dot(jnp.concatenate([hot, minute], axis=0), x, preferred_element_type=jnp.float32)
            t_buf[slot_b] = jnp.where(fresh == 1, 0.0, t_buf[slot_b]) + both[:BINS]
            total = both[BINS : BINS + 8]
            high = total.astype(jnp.bfloat16)
            low = (total - high.astype(jnp.float32)).astype(jnp.bfloat16)
            least, most = minute_extremes(x, count)
            st_buf[b] = jnp.concatenate([least, most, high, low], axis=0)
            st_copy(b).start()

            @pl.when(last == 1)
            def _():
                t_copy(b).start()

        return 0

    lax.fori_loop(0, steps, chunk, 0)

    def finish(b, _):
        st_copy(b).wait()

        @pl.when(idx_ref[4, b] == 1)
        def _():
            t_copy(b).wait()

        return 0

    lax.fori_loop(0, BLK, finish, 0)


def local_call(samples, marks, counts, series, theirs, owner_map):
    step = 8
    vmem = pl.BlockSpec(memory_space=pltpu.VMEM)
    any_ = pl.BlockSpec(memory_space=pl.ANY)
    lane = np.arange(LANES)
    live_at = np.stack([(lane // 8) * 16 + r * 8 + lane % 8 for r in (0, 1)]).astype(np.int32)
    i32, f32 = jnp.int32, jnp.float32
    return pl.pallas_call(
        functools.partial(local_kernel, step=step),
        in_specs=[any_] + [vmem] * 7,
        out_specs=[any_, any_] + [vmem] * 4,
        out_shape=[
            jax.ShapeDtypeStruct((SHARDS * CAP, BINS, LANES), f32),
            jax.ShapeDtypeStruct((SHARDS * CAP, 32, LANES), jnp.bfloat16),
            jax.ShapeDtypeStruct((PARTS, 128), i32),
            jax.ShapeDtypeStruct((PARTS, 128), i32),
            jax.ShapeDtypeStruct((SHARDS, 1, LANES), f32),
            jax.ShapeDtypeStruct((2, 1, LANES), f32),
        ],
        scratch_shapes=[
            pltpu.VMEM((BLK, SAMPLES, LANES), jnp.bfloat16),
            pltpu.VMEM((SHARDS * CAP, BINS, LANES), f32),
            pltpu.VMEM((BLK, 32, LANES), jnp.bfloat16),
            pltpu.VMEM((8, 128), i32),
            pltpu.SMEM((8, 128), i32),
            pltpu.SemaphoreType.DMA((BLK // step,)),
            pltpu.SemaphoreType.DMA((BLK,)),
            pltpu.SemaphoreType.DMA((BLK,)),
            pltpu.SemaphoreType.DMA,
        ],
        compiler_params=pltpu.CompilerParams(vmem_limit_bytes=56 * 2**20),
        name="local_stats",
    )(
        samples, marks, counts.reshape(1, BLK), series.reshape(1, BLK), theirs.reshape(1, BLK),
        owner_map.reshape(1, -1), jnp.asarray(part_positions()), jnp.asarray(live_at),
    )


def exchange_kernel(
    own_idx, prt_idx, table, stats, meta, live,
    sk_out, stats_out, meta_out, live_out,
    *scratch,
):
    own, prt, acc, out, outs, got, gots = (scratch[PARTS * i : PARTS * (i + 1)] for i in range(7))
    mine_st, mine_meta, rows_in, lbuf, lgot = scratch[7 * PARTS : 7 * PARTS + 5]
    (own_sem, d2d_send, d2d_recv, cube_send, cube_recv, st_send, st_recv, l_send, l_recv, loc_sem) = scratch[7 * PARTS + 5 :]
    shard = lax.axis_index("shard")
    y = lax.axis_index("replica")
    core = lax.rem(shard, 2)
    x = lax.rem(lax.div(shard, 2), 4)
    z = lax.div(shard, 8)
    where_at = {"x": x, "y": y, "z": z}

    def other(dim):
        axis, bit = dim
        v = where_at[axis]
        high = lax.div(v, 2)
        if bit == 0:
            mine = lax.rem(v + high, 2)
            w = v + 1 - 2 * lax.rem(v, 2)
        else:
            mine = high
            w = 3 - v
        if axis == "x":
            return {"shard": shard + (w - v) * 2, "replica": y}, mine
        if axis == "z":
            return {"shard": shard + (w - v) * 8, "replica": y}, mine
        return {"shard": shard, "replica": w}, mine

    across = [other(d) for d in DIMS]
    partner = {"shard": shard + 1 - 2 * core, "replica": y}

    barrier = pltpu.get_barrier_semaphore()

    def greet(d, _):
        pl.semaphore_signal(barrier, inc=1, device_id={"shard": lax.rem(shard + d, SHARDS), "replica": y})
        return 0

    lax.fori_loop(1, SHARDS, greet, 0)
    for d in (2, 5):
        pl.semaphore_signal(barrier, inc=1, device_id=across[d][0])
    own_copies = []
    for p in range(PARTS):
        rows = pl.ds(p * ROWS, ROWS)
        c = pltpu.make_async_copy(table.at[core, :, rows], own[p].at[pl.ds(0, BLK)], own_sem.at[p])
        c.start()
        own_copies.append(c)
    st_in = pltpu.make_async_copy(stats.at[shard], mine_st, loc_sem.at[0])
    st_in.start()
    meta_in = pltpu.make_async_copy(meta.at[shard], mine_meta, loc_sem.at[1])
    meta_in.start()
    live_in = pltpu.make_async_copy(live, rows_in, loc_sem.at[2])
    live_in.start()
    for p in range(PARTS):
        own[p][BLK] = jnp.zeros((ROWS, LANES), jnp.float32)
        prt[p][BLK] = jnp.zeros((ROWS, LANES), jnp.float32)
    pl.semaphore_wait(barrier, SHARDS + 1)

    def d2d(p):
        rows = pl.ds(p * ROWS, ROWS)
        return pltpu.make_async_remote_copy(
            table.at[1 - core, :, rows], prt[p].at[pl.ds(0, BLK)], d2d_send.at[p], d2d_recv.at[p], device_id=partner,
        )

    parts = tuple(range(PARTS))
    d2d_copies = {p: d2d(p) for p in parts}
    for p in parts:
        d2d_copies[p].start()

    def st_copy(d, dst_shard, src_slot):
        return pltpu.make_async_remote_copy(
            stats.at[dst_shard], stats_out.at[src_slot], st_send.at[0, d], st_recv.at[0, d],
            device_id={"shard": dst_shard, "replica": y},
        )

    def meta_copy(d, dst_shard, src_slot):
        return pltpu.make_async_remote_copy(
            meta.at[dst_shard], meta_out.at[src_slot], st_send.at[1, d], st_recv.at[1, d],
            device_id={"shard": dst_shard, "replica": y},
        )

    def send_stats(d, _):
        to = lax.rem(shard + d, SHARDS)
        st_copy(d, to, shard).start()
        meta_copy(d, to, shard).start()
        return 0

    lax.fori_loop(1, SHARDS, send_stats, 0)
    st_in.wait()
    st_back = pltpu.make_async_copy(mine_st, stats_out.at[shard], loc_sem.at[3])
    st_back.start()
    meta_in.wait()
    meta_back = pltpu.make_async_copy(mine_meta, meta_out.at[shard], loc_sem.at[4])
    meta_back.start()
    live_in.wait()

    def live_copy(s, src, device):
        return pltpu.make_async_remote_copy(src, lgot.at[s], l_send.at[s], l_recv.at[s], device_id=device)

    live_copies = [live_copy(0, rows_in.at[1 - core], partner)]
    live_copies[0].start()

    bases = [[None] * 7 for _ in parts]
    copies = [[None] * 6 for _ in parts]

    def encode(v):
        size = jnp.max(jnp.abs(v), axis=0, keepdims=True)
        gain = jnp.where(size > TINY, LEVELS / jnp.maximum(size, TINY), 0.0)
        code = (v * gain + 32768.5).astype(jnp.int32)
        return (code[:8] << 16) | code[8:], size

    def decode(word, size):
        unit = size * (1.0 / LEVELS)
        high = lax.shift_right_logical(word, 16).astype(jnp.float32)
        low = (word & 0xFFFF).astype(jnp.float32)
        return jnp.concatenate([(high - 32768.0) * unit, (low - 32768.0) * unit], axis=0)

    def each(n, fn):
        unroll = min(n, 8)

        def body(i, _):
            for u in range(unroll):
                fn(i * unroll + u)
            return 0

        lax.fori_loop(0, n // unroll, body, 0)

    def densify(p, lo, to=None):
        def one(i):
            e = lo + i
            v = own[p][own_idx[p, e]] + prt[p][prt_idx[p, e]]
            if to is None:
                acc[p][e] = v
            else:
                out[p][to + i], outs[p][to + i] = encode(v)

        each(64, one)

    def add_in(p, at, lo, n, to=None):
        def one(i):
            v = acc[p][at + i] + decode(got[p][lo + i], gots[p][lo + i])
            if to is None:
                acc[p][at + i] = v
            else:
                out[p][to + i], outs[p][to + i] = encode(v)

        each(n, one)

    def offset(s):
        return 128 - (128 >> s)

    def send(p, s):
        device, bit = across[ORDERS[p][s]]
        half = 64 >> s
        region = pl.ds(offset(s), half)
        both = []
        for k, (src, dst) in enumerate(((out, got), (outs, gots))):
            c = pltpu.make_async_remote_copy(
                src[p].at[region], dst[p].at[region], cube_send.at[k, p, s], cube_recv.at[k, p, s], device_id=device,
            )
            c.start()
            both.append(c)
        copies[p][s] = both
        bases[p][s + 1] = bases[p][s] + bit * half

    for p in parts:
        own_copies[p].wait()
        d2d_copies[p].wait_recv()
        bases[p][0] = 0
        bit = across[ORDERS[p][0]][1]
        densify(p, (1 - bit) * 64, 0)
        send(p, 0)
        densify(p, bit * 64)

    live_copies[0].wait_recv()
    lbuf[0] = rows_in[core] + lgot[0]
    for s in range(1, 7):
        live_copies.append(live_copy(s, lbuf.at[s - 1], across[ORDERS[0][s - 1]][0]))
        live_copies[s].start()
        for p in parts:
            for c in copies[p][s - 1]:
                c.wait_recv()
            half = 64 >> (s - 1)
            lo = offset(s - 1)
            base = bases[p][s]
            if s < 6:
                quarter = half // 2
                bit = across[ORDERS[p][s]][1]
                away = (1 - bit) * quarter
                add_in(p, base + away, lo + away, quarter, offset(s))
                send(p, s)
                add_in(p, base + bit * quarter, lo + bit * quarter, quarter)
            else:
                for k in range(2):
                    v = acc[p][base + k] + decode(got[p][lo + k], gots[p][lo + k])
                    sk_out[k, p * ROWS : (p + 1) * ROWS, :] = v
        live_copies[s].wait_recv()
        lbuf[s] = lbuf[s - 1] + lgot[s]
    live_out[...] = lbuf[6]

    def wait_stats(d, _):
        came = lax.rem(shard - d + SHARDS, SHARDS)
        st_copy(d, shard, came).wait_recv()
        meta_copy(d, shard, came).wait_recv()
        return 0

    lax.fori_loop(1, SHARDS, wait_stats, 0)

    def wait_sends(d, _):
        to = lax.rem(shard + d, SHARDS)
        st_copy(d, to, shard).wait_send()
        meta_copy(d, to, shard).wait_send()
        return 0

    lax.fori_loop(1, SHARDS, wait_sends, 0)
    st_back.wait()
    meta_back.wait()
    for c in live_copies:
        c.wait_send()
    for p in parts:
        d2d_copies[p].wait_send()
        for s in range(6):
            for c in copies[p][s]:
                c.wait_send()


def exchange_call(own_idx, prt_idx, table, stats, meta, live):
    any_ = pl.BlockSpec(memory_space=pl.ANY)
    vmem = pl.BlockSpec(memory_space=pltpu.VMEM)
    smem = pl.BlockSpec(memory_space=pltpu.SMEM)
    f32 = jnp.float32
    scratch = (
        [pltpu.VMEM((BLK + 1, ROWS, LANES), f32)] * (2 * PARTS)
        + [pltpu.VMEM((128, ROWS, LANES), f32)] * PARTS
        + [pltpu.VMEM((126, 8, LANES), jnp.int32)] * PARTS
        + [pltpu.VMEM((126, 1, LANES), f32)] * PARTS
        + [pltpu.VMEM((126, 8, LANES), jnp.int32)] * PARTS
        + [pltpu.VMEM((126, 1, LANES), f32)] * PARTS
        + [
            pltpu.VMEM((CAP, 32, LANES), jnp.bfloat16),
            pltpu.VMEM((1, LANES), f32),
            pltpu.VMEM((2, 1, LANES), f32),
            pltpu.VMEM((7, 1, LANES), f32),
            pltpu.VMEM((7, 1, LANES), f32),
        ]
        + [
            pltpu.SemaphoreType.DMA((PARTS,)),
            pltpu.SemaphoreType.DMA((PARTS,)),
            pltpu.SemaphoreType.DMA((PARTS,)),
            pltpu.SemaphoreType.DMA((2, PARTS, 6)),
            pltpu.SemaphoreType.DMA((2, PARTS, 6)),
            pltpu.SemaphoreType.DMA((2, SHARDS)),
            pltpu.SemaphoreType.DMA((2, SHARDS)),
            pltpu.SemaphoreType.DMA((7,)),
            pltpu.SemaphoreType.DMA((7,)),
            pltpu.SemaphoreType.DMA((5,)),
        ]
    )
    return pl.pallas_call(
        exchange_kernel,
        in_specs=[smem, smem, any_, any_, any_, any_],
        out_specs=[vmem, any_, any_, vmem],
        out_shape=[
            jax.ShapeDtypeStruct((2, BINS, LANES), f32),
            jax.ShapeDtypeStruct((SHARDS, CAP, 32, LANES), jnp.bfloat16),
            jax.ShapeDtypeStruct((SHARDS, 1, LANES), f32),
            jax.ShapeDtypeStruct((1, LANES), f32),
        ],
        scratch_shapes=scratch,
        compiler_params=pltpu.CompilerParams(
            collective_id=0, has_side_effects=True, vmem_limit_bytes=56 * 2**20
        ),
        name="exchange",
    )(own_idx, prt_idx, table, stats, meta, live)


def finish_kernel(counts, stats, sk_ref, live_ref, cold, sk_out, live_out, st_buf, cold_buf, in_sem, out_sem, *, step):
    steps = SHARDS * CAP // step
    for i in range(steps):
        part = pl.ds(i * step, step)
        pltpu.make_async_copy(stats.at[part], st_buf.at[part], in_sem.at[i]).start()
    minute = lax.broadcasted_iota(jnp.int32, (8, LANES), 0).astype(jnp.float32) * 60.0
    sk_out[...] = sk_ref[...]
    place = lax.div(lax.axis_index("shard"), 2) * 8 + lax.axis_index("replica") * 2
    lane = lax.broadcasted_iota(jnp.int32, (1, LANES), 1)
    for k in range(2):
        live_out[k] = jnp.sum(jnp.where(lane == place + k, live_ref[...], 0.0))
    for i in range(steps):
        part = pl.ds(i * step, step)
        pltpu.make_async_copy(stats.at[part], st_buf.at[part], in_sem.at[i]).wait()

        def group(g, _):
            source = i * (step // CAP) + g
            for c in range(CAP):
                at = source * CAP + c
                count = jnp.clip(counts[source, 0, c] - minute, 0.0, 60.0)
                filled = count > 0
                st = st_buf[at].astype(jnp.float32)
                cold_buf[at, 0] = jnp.where(filled, st[0:8], 0.0)
                cold_buf[at, 1] = jnp.where(filled, st[8:16], 0.0)
                cold_buf[at, 2] = jnp.where(filled, st[16:24] + st[24:32], 0.0)
                cold_buf[at, 3] = count
            return 0

        lax.fori_loop(0, step // CAP, group, 0)
        pltpu.make_async_copy(cold_buf.at[part], cold.at[part], out_sem.at[i]).start()
    for i in range(steps):
        part = pl.ds(i * step, step)
        pltpu.make_async_copy(cold_buf.at[part], cold.at[part], out_sem.at[i]).wait()


def finish_call(counts, stats, sketches, live):
    step = 32
    vmem = pl.BlockSpec(memory_space=pltpu.VMEM)
    smem = pl.BlockSpec(memory_space=pltpu.SMEM)
    any_ = pl.BlockSpec(memory_space=pl.ANY)
    return pl.pallas_call(
        functools.partial(finish_kernel, step=step),
        in_specs=[smem, any_, vmem, vmem],
        out_specs=[any_, vmem, smem],
        out_shape=[
            jax.ShapeDtypeStruct((SHARDS * CAP, 4, 8, LANES), jnp.float32),
            jax.ShapeDtypeStruct((2, BINS, LANES), jnp.float32),
            jax.ShapeDtypeStruct((2,), jnp.float32),
        ],
        scratch_shapes=[
            pltpu.VMEM((SHARDS * CAP, 32, LANES), jnp.bfloat16),
            pltpu.VMEM((SHARDS * CAP, 4, 8, LANES), jnp.float32),
            pltpu.SemaphoreType.DMA((SHARDS * CAP // step,)),
            pltpu.SemaphoreType.DMA((SHARDS * CAP // step,)),
        ],
        name="finish",
    )(counts, stats, sketches, live)


def body(samples, counts, buckets, block_series, owner_map):
    swap = [(i, i ^ 1) for i in range(SHARDS)]
    theirs = lax.ppermute(block_series, "shard", swap)
    table, stats, own_idx, prt_idx, meta, live = local_call(samples, buckets, counts, block_series, theirs, owner_map)
    sk, st, got_counts, got_live = exchange_call(
        own_idx, prt_idx, table.reshape(2, BLK, BINS, LANES), stats.reshape(SHARDS, CAP, 32, LANES), meta, live,
    )
    cold, sketches, live_rows = finish_call(got_counts, st.reshape(SHARDS * CAP, 32, LANES), sk, got_live)
    return cold.reshape(1, 1, SHARDS * CAP, 4, 8, LANES), sketches, live_rows


def solution(mesh):
    return jax.shard_map(
        body,
        mesh=mesh,
        in_specs=(
            P(("shard", "replica"), None, None),
            P(("shard", "replica")),
            P(("shard", "replica"), None),
            P(("shard", "replica")),
            P(),
        ),
        out_specs=(
            P("shard", "replica", None, None, None, None),
            P(("shard", "replica"), None, None),
            P(("shard", "replica")),
        ),
        check_vma=False,
    )
```

```python
import functools

import jax
import jax.numpy as jnp
import numpy as np
from jax import lax
from jax.experimental import pallas as pl
from jax.experimental.pallas import tpu as pltpu
from jax.sharding import PartitionSpec as P

BINS = 128
LANES = 128
SAMPLES = 480
BLK = 64
SHARDS = 32
REPLICAS = 4
CAP = 4
DIMS = (("x", 0), ("z", 0), ("y", 0), ("x", 1), ("z", 1), ("y", 1))
ORDERS = (
    (5, 2, 4, 0, 3, 1), (5, 4, 1, 2, 0, 3), (2, 5, 1, 3, 4, 0), (0, 1, 4, 3, 5, 2),
    (2, 0, 3, 4, 1, 5), (3, 2, 5, 4, 1, 0), (4, 3, 0, 5, 2, 1), (1, 5, 2, 0, 3, 4),
)
PARTS = len(ORDERS)
ROWS = BINS // PARTS
LEVELS = 32766.0
TINY = 1e-33
GRAY = {(0, 0): 0, (0, 1): 1, (1, 1): 2, (1, 0): 3}


HALVINGS = 3


def last_groups(p):
    tail = ORDERS[p][HALVINGS:]
    return [tuple(d for k, d in enumerate(tail) if m >> k & 1) for m in range(1, 8)]


def off_plane():
    dims = {(order[s],) for order in ORDERS for s in range(HALVINGS)}
    dims |= {tuple(sorted(g)) for p in range(PARTS) for g in last_groups(p)}
    return tuple(sorted(g for g in dims if any(DIMS[d][0] == "y" for d in g)))


OFF_PLANE = off_plane()


def part_positions():
    table = np.zeros((PARTS, 128), np.int32)
    for p, order in enumerate(ORDERS):
        for i in range(128):
            bits = {DIMS[d]: (i >> (6 - s)) & 1 for s, d in enumerate(order)}
            x, y, z = (GRAY[(bits[(a, 1)], bits[(a, 0)])] for a in "xyz")
            table[p, i] = (z * 4 + x) * 16 + y * 2 + (i & 1)
    return table


def minute_extremes(x, count):
    sub16 = lax.broadcasted_iota(jnp.int16, (16, LANES), 0)
    sub = lax.broadcasted_iota(jnp.int32, (8, LANES), 0)
    least = jnp.zeros((8, LANES), jnp.float32)
    most = jnp.zeros((8, LANES), jnp.float32)
    inf = jnp.bfloat16(jnp.inf)
    for q in range(2):
        lo = [None] * 4
        hi = [None] * 4
        for v in range(15):
            at_row = 240 * q + 16 * v
            val = x[at_row : at_row + 16]
            ok = sub16 < jnp.full((16, LANES), jnp.clip(count - at_row, 0, 16), jnp.int32).astype(jnp.int16)
            small, large = jnp.where(ok, val, inf), jnp.where(ok, val, -inf)
            for h in range(4):
                a, b = 60 * h - 16 * v, 60 * h + 60 - 16 * v
                if b <= 0 or a >= 16:
                    continue
                s, g = small, large
                if a > 0:
                    s, g = jnp.where(sub16 >= a, s, inf), jnp.where(sub16 >= a, g, -inf)
                if b < 16:
                    s, g = jnp.where(sub16 < b, s, inf), jnp.where(sub16 < b, g, -inf)
                lo[h] = s if lo[h] is None else jnp.minimum(lo[h], s)
                hi[h] = g if hi[h] is None else jnp.maximum(hi[h], g)
        for h in range(4):
            m = 4 * q + h
            least = jnp.where(sub == m, jnp.min(lo[h].astype(jnp.float32), axis=0, keepdims=True), least)
            most = jnp.where(sub == m, jnp.max(hi[h].astype(jnp.float32), axis=0, keepdims=True), most)
    return least.astype(jnp.bfloat16), most.astype(jnp.bfloat16)


def iota(shape, dim):
    return lax.broadcasted_iota(jnp.int32, shape, dim)


def routing(series_row, map_row):
    sub, lane = iota((BLK, BLK), 0), iota((BLK, BLK), 1)
    eye = sub == lane

    def row(col):
        return jnp.sum(jnp.where(eye, col, 0), axis=0, keepdims=True)

    series = jnp.sum(jnp.where(eye, series_row, 0), axis=1, keepdims=True)
    pos = jnp.sum(jnp.where(iota((BLK, 256), 1) == series, map_row, 0), axis=1, keepdims=True)
    pos_r = row(pos)
    owner, owner_r = pos >> 3, pos_r >> 3
    rank = jnp.sum(jnp.where((owner == owner_r) & (lane < sub), 1, 0), axis=1, keepdims=True)
    return pos, owner, rank, pos_r, owner_r


def flip(v, bit):
    return v + 1 - 2 * lax.rem(v, 2) if bit == 0 else 3 - v


def exchange_kernel(
    samples, marks_ref, counts_ref, series_ref, theirs_ref, map_ref, target_ref, live_at,
    sk_out, stats_out, meta_out, live_out,
    x_buf, own, prt, st_nat, st_slots, meta_v, live_v, idx_v, idx_ref, lbuf, lgot,
    in_sem, idx_sem, d2d_send, d2d_recv, cube_send, cube_recv, st_send, st_recv, l_send, l_recv, loc_sem,
    *rest, step,
):
    acc, out, outs, got, gots = (rest[PARTS * i : PARTS * (i + 1)] for i in range(5))
    steps = BLK // step
    parts = tuple(range(PARTS))

    def in_copy(i):
        part = pl.ds(i * step, step)
        return pltpu.make_async_copy(samples.at[part], x_buf.at[part], in_sem.at[i])

    for i in range(steps):
        in_copy(i).start()

    shard = lax.axis_index("shard")
    y = lax.axis_index("replica")
    core = lax.rem(shard, 2)
    x = lax.rem(lax.div(shard, 2), 4)
    z = lax.div(shard, 8)

    def across(dims):
        v = {"x": x, "y": y, "z": z}
        for d in dims:
            axis, bit = DIMS[d]
            v[axis] = flip(v[axis], bit)
        return {"shard": v["z"] * 8 + v["x"] * 2 + core, "replica": v["y"]}

    def bit_of(d):
        axis, bit = DIMS[d]
        v = {"x": x, "y": y, "z": z}[axis]
        high = lax.div(v, 2)
        return high if bit == 1 else lax.rem(v + high, 2)

    bits = [bit_of(d) for d in range(6)]
    partner = {"shard": shard + 1 - 2 * core, "replica": y}

    barrier = pltpu.get_barrier_semaphore()

    def greet(d, _):
        pl.semaphore_signal(barrier, inc=1, device_id={"shard": lax.rem(shard + d, SHARDS), "replica": y})
        return 0

    lax.fori_loop(1, SHARDS, greet, 0)
    for dims in OFF_PLANE:
        pl.semaphore_signal(barrier, inc=1, device_id=across(dims))

    map_row = map_ref[...]
    pos, owner, rank, pos_r, owner_r = routing(series_ref[...], map_row)
    sub, lane = iota((BLK, BLK), 0), iota((BLK, BLK), 1)
    before = jnp.max(jnp.where((pos == pos_r) & (sub < lane), sub, -1), axis=0, keepdims=True)
    idx_v[0:1, 0:BLK] = jnp.where(before < 0, BLK, jnp.minimum(before, BLK))
    idx_v[1:2, 0:BLK] = counts_ref[...]
    block = iota((BLK, LANES), 0)
    filled = iota((BLK, LANES), 1) == owner * CAP + rank
    idx_v[2:3, :] = jnp.clip(jnp.max(jnp.where(filled, block, 0), axis=0, keepdims=True), 0, BLK - 1)
    their_pos = routing(theirs_ref[...], map_row)[0]
    for p in parts:
        want = target_ref[p : p + 1, :] + core * 8
        for k, at in enumerate((pos, their_pos)):
            hit = jnp.max(jnp.where(at == want, block, -1), axis=0, keepdims=True)
            row = 8 + k * PARTS + p
            idx_v[row : row + 1, :] = jnp.where(hit < 0, BLK, jnp.minimum(hit, BLK))
    idx_copy = pltpu.make_async_copy(idx_v, idx_ref, idx_sem)
    idx_copy.start()
    counts_row = counts_ref[...].astype(jnp.float32)
    counts_col = jnp.sum(jnp.where(sub == lane, counts_row, 0.0), axis=1, keepdims=True)
    for r in range(2):
        at = live_at[r : r + 1, :]
        live_v[r] = jnp.sum(jnp.where(pos == at, counts_col, 0.0), axis=0, keepdims=True)
    pick = jnp.where(iota((SHARDS, BLK), 0) == owner_r, 1.0, 0.0)
    put = jnp.where(iota((BLK, LANES), 1) == rank, counts_col, 0.0)
    meta = jnp.dot(pick, put, precision=lax.Precision.HIGHEST, preferred_element_type=jnp.float32)
    for o in range(SHARDS):
        meta_v[o] = meta[o : o + 1, :]
    own[BLK] = jnp.zeros((BINS, LANES), jnp.float32)
    prt[BLK] = jnp.zeros((BINS, LANES), jnp.float32)
    idx_copy.wait()
    pl.semaphore_wait(barrier, SHARDS - 1 + len(OFF_PLANE))

    def live_copy(s, src, device):
        return pltpu.make_async_remote_copy(src, lgot.at[s], l_send.at[s], l_recv.at[s], device_id=device)

    live_copies = [live_copy(0, live_v.at[1 - core], partner)]
    live_copies[0].start()

    row_at = lax.broadcasted_iota(jnp.int32, (1, SAMPLES), 1)
    bins = lax.broadcasted_iota(jnp.int32, (BINS, SAMPLES), 0)
    first_row = lax.broadcasted_iota(jnp.int32, (16, SAMPLES), 0) * 60

    def d2d(i):
        part = pl.ds(i * step, step)
        return pltpu.make_async_remote_copy(
            own.at[part], prt.at[part], d2d_send.at[i], d2d_recv.at[i], device_id=partner
        )

    def chunk(i, _):
        in_copy(i).wait()
        for j in range(step):
            b = i * step + j
            before, count = idx_ref[0, b], idx_ref[1, b]
            x = x_buf[b]
            live = row_at < count
            marks = jnp.where(live, marks_ref[pl.ds(b, 1), :], -1)
            hot = jnp.where(bins == marks, 1.0, 0.0).astype(jnp.bfloat16)
            at = jnp.where(live, row_at, -1)
            minute = jnp.where((at >= first_row) & (at < first_row + 60), 1.0, 0.0).astype(jnp.bfloat16)
            both = jnp.dot(jnp.concatenate([hot, minute], axis=0), x, preferred_element_type=jnp.float32)
            own[b] = own[before] + both[:BINS]
            total = both[BINS : BINS + 8]
            high = total.astype(jnp.bfloat16)
            low = (total - high.astype(jnp.float32)).astype(jnp.bfloat16)
            least, most = minute_extremes(x, count)
            st_nat[b] = jnp.concatenate([least, most, high, low], axis=0)
        d2d(i).start()
        return 0

    lax.fori_loop(0, steps, chunk, 0)

    def place(o, _):
        for c in range(CAP):
            st_slots[o, c] = st_nat[idx_ref[2, o * CAP + c]]
        return 0

    lax.fori_loop(0, SHARDS, place, 0)

    def st_copies(d, to, slot):
        device = {"shard": to, "replica": y}
        return [
            pltpu.make_async_remote_copy(
                src.at[to], dst.at[slot], st_send.at[k, d], st_recv.at[k, d], device_id=device
            )
            for k, (src, dst) in enumerate(((st_slots, stats_out), (meta_v, meta_out)))
        ]

    def send_stats(d, _):
        for c in st_copies(d, lax.rem(shard + d, SHARDS), shard):
            c.start()
        return 0

    lax.fori_loop(1, SHARDS, send_stats, 0)
    kept = [
        pltpu.make_async_copy(st_slots.at[shard], stats_out.at[shard], loc_sem.at[0]),
        pltpu.make_async_copy(meta_v.at[shard], meta_out.at[shard], loc_sem.at[1]),
    ]
    for c in kept:
        c.start()

    bases = [[0] * (HALVINGS + 1) for _ in parts]
    copies = [[] for _ in parts]

    def encode(v):
        size = jnp.max(jnp.abs(v), axis=0, keepdims=True)
        gain = jnp.where(size > TINY, LEVELS / jnp.maximum(size, TINY), 0.0)
        code = (v * gain + 32768.5).astype(jnp.int32)
        return (code[:8] << 16) | code[8:], size

    def decode(word, size):
        unit = size * (1.0 / LEVELS)
        high = lax.shift_right_logical(word, 16).astype(jnp.float32)
        low = (word & 0xFFFF).astype(jnp.float32)
        return jnp.concatenate([(high - 32768.0) * unit, (low - 32768.0) * unit], axis=0)

    def each(n, fn):
        unroll = min(n, 8)

        def body(i, _):
            for u in range(unroll):
                fn(i * unroll + u)
            return 0

        lax.fori_loop(0, n // unroll, body, 0)

    def densify(p, lo, to=None):
        rows = pl.ds(p * ROWS, ROWS)

        def one(i):
            e = lo + i
            v = own[idx_ref[8 + p, e], rows] + prt[idx_ref[8 + PARTS + p, e], rows]
            if to is None:
                acc[p][e] = v
            else:
                out[p][to + i], outs[p][to + i] = encode(v)

        each(64, one)

    def add_in(p, at, lo, n, to=None):
        def one(i):
            v = acc[p][at + i] + decode(got[p][lo + i], gots[p][lo + i])
            if to is None:
                acc[p][at + i] = v
            else:
                out[p][to + i], outs[p][to + i] = encode(v)

        each(n, one)

    def offset(s):
        return 128 - (128 >> s)

    def send(p, slot, lo, n, device):
        region = pl.ds(lo, n)
        both = [
            pltpu.make_async_remote_copy(
                src[p].at[region], dst[p].at[region], cube_send.at[k, p, slot], cube_recv.at[k, p, slot], device_id=device,
            )
            for k, (src, dst) in enumerate(((out, got), (outs, gots)))
        ]
        for c in both:
            c.start()
        copies[p].append(both)

    def halve(p, s):
        d = ORDERS[p][s]
        half = 64 >> s
        send(p, s, offset(s), half, across((d,)))
        bases[p][s + 1] = bases[p][s] + bits[d] * half

    for i in range(steps):
        d2d(i).wait_recv()
    for p in parts:
        bit = bits[ORDERS[p][0]]
        densify(p, (1 - bit) * 64, 0)
        halve(p, 0)
        densify(p, bit * 64)

    live_copies[0].wait_recv()
    lbuf[0] = live_v[core] + lgot[0]
    for s in range(1, HALVINGS + 1):
        live_copies.append(live_copy(s, lbuf.at[s - 1], across((ORDERS[0][s - 1],))))
        live_copies[s].start()
        half = 64 >> (s - 1)
        lo = offset(s - 1)
        for p in parts:
            for c in copies[p][s - 1]:
                c.wait_recv()
            base = bases[p][s]
            if s < HALVINGS:
                quarter = half // 2
                bit = bits[ORDERS[p][s]]
                away = (1 - bit) * quarter
                add_in(p, base + away, lo + away, quarter, offset(s))
                halve(p, s)
                add_in(p, base + bit * quarter, lo + bit * quarter, quarter)
            else:
                add_in(p, base, lo, half)
                for m, dims in enumerate(last_groups(p), 1):
                    theirs = base
                    for w, d in zip((half // 2, half // 4, half // 8), ORDERS[p][HALVINGS:]):
                        theirs = theirs + (1 - bits[d] if d in dims else bits[d]) * w
                    spot = offset(HALVINGS) + (m - 1) * 2
                    for k in range(2):
                        out[p][spot + k], outs[p][spot + k] = encode(acc[p][theirs + k])
                    send(p, HALVINGS + m - 1, spot, 2, across(dims))
        live_copies[s].wait_recv()
        lbuf[s] = lbuf[s - 1] + lgot[s]
    for m, dims in enumerate(last_groups(0), 1):
        c = live_copy(HALVINGS + m, lbuf.at[HALVINGS], across(dims))
        c.start()
        live_copies.append(c)
    for p in parts:
        mine = bases[p][HALVINGS]
        for w, d in zip((8, 4, 2), ORDERS[p][HALVINGS:]):
            mine = mine + bits[d] * w
        v = [acc[p][mine + k] for k in range(2)]
        for m in range(1, 8):
            for c in copies[p][HALVINGS + m - 1]:
                c.wait_recv()
            spot = offset(HALVINGS) + (m - 1) * 2
            v = [v[k] + decode(got[p][spot + k], gots[p][spot + k]) for k in range(2)]
        for k in range(2):
            sk_out[k, p * ROWS : (p + 1) * ROWS, :] = v[k]
    total = lbuf[HALVINGS]
    for m in range(1, 8):
        live_copies[HALVINGS + m].wait_recv()
        total = total + lgot[HALVINGS + m]
    live_out[...] = total

    def wait_stats(d, _):
        for c in st_copies(d, shard, lax.rem(shard - d + SHARDS, SHARDS)):
            c.wait_recv()
        return 0

    lax.fori_loop(1, SHARDS, wait_stats, 0)

    def wait_sends(d, _):
        for c in st_copies(d, lax.rem(shard + d, SHARDS), shard):
            c.wait_send()
        return 0

    lax.fori_loop(1, SHARDS, wait_sends, 0)
    for c in kept:
        c.wait()
    for c in live_copies:
        c.wait_send()
    for i in range(steps):
        d2d(i).wait_send()
    for p in parts:
        for both in copies[p]:
            for c in both:
                c.wait_send()


def exchange_call(samples, marks, counts, series, theirs, owner_map):
    step = 8
    vmem = pl.BlockSpec(memory_space=pltpu.VMEM)
    any_ = pl.BlockSpec(memory_space=pl.ANY)
    lane = np.arange(LANES)
    live_at = np.stack([(lane // 8) * 16 + r * 8 + lane % 8 for r in (0, 1)]).astype(np.int32)
    i32, f32, bf16 = jnp.int32, jnp.float32, jnp.bfloat16
    dma = pltpu.SemaphoreType.DMA
    scratch = [
        pltpu.VMEM((BLK, SAMPLES, LANES), bf16),
        pltpu.VMEM((BLK + 1, BINS, LANES), f32),
        pltpu.VMEM((BLK + 1, BINS, LANES), f32),
        pltpu.VMEM((BLK, 32, LANES), bf16),
        pltpu.VMEM((SHARDS, CAP, 32, LANES), bf16),
        pltpu.VMEM((SHARDS, 1, LANES), f32),
        pltpu.VMEM((2, 1, LANES), f32),
        pltpu.VMEM((8 + 2 * PARTS, 128), i32),
        pltpu.SMEM((8 + 2 * PARTS, 128), i32),
        pltpu.VMEM((HALVINGS + 1, 1, LANES), f32),
        pltpu.VMEM((HALVINGS + 8, 1, LANES), f32),
        dma((BLK // step,)),
        dma,
        dma((BLK // step,)),
        dma((BLK // step,)),
        dma((2, PARTS, HALVINGS + 7)),
        dma((2, PARTS, HALVINGS + 7)),
        dma((2, SHARDS)),
        dma((2, SHARDS)),
        dma((HALVINGS + 8,)),
        dma((HALVINGS + 8,)),
        dma((2,)),
    ]
    scratch += [pltpu.VMEM((128, ROWS, LANES), f32)] * PARTS
    scratch += ([pltpu.VMEM((126, 8, LANES), i32)] * PARTS + [pltpu.VMEM((126, 1, LANES), f32)] * PARTS) * 2
    return pl.pallas_call(
        functools.partial(exchange_kernel, step=step),
        in_specs=[any_] + [vmem] * 7,
        out_specs=[vmem, any_, any_, vmem],
        out_shape=[
            jax.ShapeDtypeStruct((2, BINS, LANES), f32),
            jax.ShapeDtypeStruct((SHARDS, CAP, 32, LANES), bf16),
            jax.ShapeDtypeStruct((SHARDS, 1, LANES), f32),
            jax.ShapeDtypeStruct((1, LANES), f32),
        ],
        scratch_shapes=scratch,
        compiler_params=pltpu.CompilerParams(
            collective_id=0, has_side_effects=True, vmem_limit_bytes=60 * 2**20
        ),
        name="exchange",
    )(
        samples, marks, counts.reshape(1, BLK), series.reshape(1, BLK), theirs.reshape(1, BLK),
        owner_map.reshape(1, -1), jnp.asarray(part_positions()), jnp.asarray(live_at),
    )


def finish_kernel(counts, stats, sk_ref, live_ref, cold, sk_out, live_out, st_buf, cold_buf, in_sem, out_sem, *, step):
    steps = SHARDS * CAP // step
    for i in range(steps):
        part = pl.ds(i * step, step)
        pltpu.make_async_copy(stats.at[part], st_buf.at[part], in_sem.at[i]).start()
    minute = lax.broadcasted_iota(jnp.int32, (8, LANES), 0).astype(jnp.float32) * 60.0
    sk_out[...] = sk_ref[...]
    place = lax.div(lax.axis_index("shard"), 2) * 8 + lax.axis_index("replica") * 2
    lane = lax.broadcasted_iota(jnp.int32, (1, LANES), 1)
    for k in range(2):
        live_out[k] = jnp.sum(jnp.where(lane == place + k, live_ref[...], 0.0))
    for i in range(steps):
        part = pl.ds(i * step, step)
        pltpu.make_async_copy(stats.at[part], st_buf.at[part], in_sem.at[i]).wait()

        def group(g, _):
            source = i * (step // CAP) + g
            for c in range(CAP):
                at = source * CAP + c
                count = jnp.clip(counts[source, 0, c] - minute, 0.0, 60.0)
                filled = count > 0
                st = st_buf[at].astype(jnp.float32)
                cold_buf[at, 0] = jnp.where(filled, st[0:8], 0.0)
                cold_buf[at, 1] = jnp.where(filled, st[8:16], 0.0)
                cold_buf[at, 2] = jnp.where(filled, st[16:24] + st[24:32], 0.0)
                cold_buf[at, 3] = count
            return 0

        lax.fori_loop(0, step // CAP, group, 0)
        pltpu.make_async_copy(cold_buf.at[part], cold.at[part], out_sem.at[i]).start()
    for i in range(steps):
        part = pl.ds(i * step, step)
        pltpu.make_async_copy(cold_buf.at[part], cold.at[part], out_sem.at[i]).wait()


def finish_call(counts, stats, sketches, live):
    step = 32
    vmem = pl.BlockSpec(memory_space=pltpu.VMEM)
    smem = pl.BlockSpec(memory_space=pltpu.SMEM)
    any_ = pl.BlockSpec(memory_space=pl.ANY)
    return pl.pallas_call(
        functools.partial(finish_kernel, step=step),
        in_specs=[smem, any_, vmem, vmem],
        out_specs=[any_, vmem, smem],
        out_shape=[
            jax.ShapeDtypeStruct((SHARDS * CAP, 4, 8, LANES), jnp.float32),
            jax.ShapeDtypeStruct((2, BINS, LANES), jnp.float32),
            jax.ShapeDtypeStruct((2,), jnp.float32),
        ],
        scratch_shapes=[
            pltpu.VMEM((SHARDS * CAP, 32, LANES), jnp.bfloat16),
            pltpu.VMEM((SHARDS * CAP, 4, 8, LANES), jnp.float32),
            pltpu.SemaphoreType.DMA((SHARDS * CAP // step,)),
            pltpu.SemaphoreType.DMA((SHARDS * CAP // step,)),
        ],
        name="finish",
    )(counts, stats, sketches, live)


def body(samples, counts, buckets, block_series, owner_map):
    swap = [(i, i ^ 1) for i in range(SHARDS)]
    theirs = lax.ppermute(block_series, "shard", swap)
    sk, st, got_counts, got_live = exchange_call(samples, buckets, counts, block_series, theirs, owner_map)
    cold, sketches, live_rows = finish_call(got_counts, st.reshape(SHARDS * CAP, 32, LANES), sk, got_live)
    return cold.reshape(1, 1, SHARDS * CAP, 4, 8, LANES), sketches, live_rows


def solution(mesh):
    return jax.shard_map(
        body,
        mesh=mesh,
        in_specs=(
            P(("shard", "replica"), None, None),
            P(("shard", "replica")),
            P(("shard", "replica"), None),
            P(("shard", "replica")),
            P(),
        ),
        out_specs=(
            P("shard", "replica", None, None, None, None),
            P(("shard", "replica"), None, None),
            P(("shard", "replica")),
        ),
        check_vma=False,
    )
```

```python
import functools

import jax
import jax.numpy as jnp
import numpy as np
from jax import lax
from jax.experimental import pallas as pl
from jax.experimental.pallas import tpu as pltpu
from jax.sharding import PartitionSpec as P

BINS = 128
LANES = 128
SAMPLES = 480
BLK = 64
SHARDS = 32
REPLICAS = 4
CAP = 4
DIMS = (("x", 0), ("z", 0), ("y", 0), ("x", 1), ("z", 1), ("y", 1))
GROUPS = (
    ((3, 0, 5), (0, 3, 5)), ((4, 5, 2), (5, 2, 4)), ((1, 0, 3), (0, 3, 1)), ((3, 5, 1), (3, 1, 5)),
    ((2, 0, 4), (4, 2, 0)), ((5, 0, 2), (5, 2, 0)), ((1, 2, 4), (4, 2, 1)), ((2, 5, 4), (5, 2, 4)),
)
EVENTS = (
    (0, 0, 1), (0, 1, 1), (1, 0, 1), (1, 1, 1), (2, 0, 1), (3, 0, 1), (2, 1, 1), (4, 0, 1), (4, 1, 1), (5, 0, 1),
    (0, 0, 2), (6, 0, 1), (3, 1, 1), (2, 0, 2), (7, 0, 1), (6, 1, 1), (5, 1, 1), (0, 1, 2), (1, 1, 2), (4, 0, 2),
    (2, 1, 2), (4, 1, 2), (7, 1, 1), (6, 0, 2), (1, 0, 2), (6, 1, 2), (3, 0, 2), (5, 1, 2), (0, 0, 3), (5, 0, 2),
    (3, 1, 2), (7, 1, 2), (1, 1, 3), (7, 0, 2), (2, 1, 3), (1, 0, 3), (4, 0, 3), (0, 1, 3), (6, 1, 3), (6, 0, 3),
    (5, 0, 3), (3, 0, 3), (2, 0, 3), (4, 1, 3), (3, 1, 3), (7, 1, 3), (5, 1, 3), (7, 0, 3),
)
TAILS = tuple(tuple(d for d in range(6) if d not in g[0]) for g in GROUPS)
PARTS = len(GROUPS)
ROWS = BINS // PARTS
LIMIT = 6.0
LEVELS = 32766.0
TINY = 1e-33
GRAY = {(0, 0): 0, (0, 1): 1, (1, 1): 2, (1, 0): 3}


HALVINGS = 3


def last_groups(p):
    return [tuple(d for k, d in enumerate(TAILS[p]) if m >> k & 1) for m in range(1, 8)]


def off_plane():
    dims = {(d,) for g in GROUPS for d in g[0]}
    dims |= {tuple(sorted(g)) for p in range(PARTS) for g in last_groups(p)}
    return tuple(sorted(g for g in dims if any(DIMS[d][0] == "y" for d in g)))


OFF_PLANE = off_plane()


def part_positions():
    table = np.zeros((PARTS, 128), np.int32)
    for p in range(PARTS):
        for k in range(2):
            order = GROUPS[p][k] + TAILS[p]
            for i in range(64):
                bits = {DIMS[d]: (i >> (5 - s)) & 1 for s, d in enumerate(order)}
                x, y, z = (GRAY[(bits[(a, 1)], bits[(a, 0)])] for a in "xyz")
                table[p, k * 64 + i] = (z * 4 + x) * 16 + y * 2 + k
    return table


def minute_extremes(x, count):
    sub16 = lax.broadcasted_iota(jnp.int16, (16, LANES), 0)
    sub = lax.broadcasted_iota(jnp.int32, (8, LANES), 0)
    least = jnp.zeros((8, LANES), jnp.float32)
    most = jnp.zeros((8, LANES), jnp.float32)
    inf = jnp.bfloat16(jnp.inf)
    for q in range(2):
        lo = [None] * 4
        hi = [None] * 4
        for v in range(15):
            at_row = 240 * q + 16 * v
            val = x[at_row : at_row + 16]
            ok = sub16 < jnp.full((16, LANES), jnp.clip(count - at_row, 0, 16), jnp.int32).astype(jnp.int16)
            small, large = jnp.where(ok, val, inf), jnp.where(ok, val, -inf)
            for h in range(4):
                a, b = 60 * h - 16 * v, 60 * h + 60 - 16 * v
                if b <= 0 or a >= 16:
                    continue
                s, g = small, large
                if a > 0:
                    s, g = jnp.where(sub16 >= a, s, inf), jnp.where(sub16 >= a, g, -inf)
                if b < 16:
                    s, g = jnp.where(sub16 < b, s, inf), jnp.where(sub16 < b, g, -inf)
                lo[h] = s if lo[h] is None else jnp.minimum(lo[h], s)
                hi[h] = g if hi[h] is None else jnp.maximum(hi[h], g)
        for h in range(4):
            m = 4 * q + h
            least = jnp.where(sub == m, jnp.min(lo[h].astype(jnp.float32), axis=0, keepdims=True), least)
            most = jnp.where(sub == m, jnp.max(hi[h].astype(jnp.float32), axis=0, keepdims=True), most)
    return least.astype(jnp.bfloat16), most.astype(jnp.bfloat16)


def iota(shape, dim):
    return lax.broadcasted_iota(jnp.int32, shape, dim)


def routing(series_row, map_row):
    sub, lane = iota((BLK, BLK), 0), iota((BLK, BLK), 1)
    eye = sub == lane

    def row(col):
        return jnp.sum(jnp.where(eye, col, 0), axis=0, keepdims=True)

    series = jnp.sum(jnp.where(eye, series_row, 0), axis=1, keepdims=True)
    pos = jnp.sum(jnp.where(iota((BLK, 256), 1) == series, map_row, 0), axis=1, keepdims=True)
    pos_r = row(pos)
    owner, owner_r = pos >> 3, pos_r >> 3
    rank = jnp.sum(jnp.where((owner == owner_r) & (lane < sub), 1, 0), axis=1, keepdims=True)
    return pos, owner, rank, pos_r, owner_r


def flip(v, bit):
    return v + 1 - 2 * lax.rem(v, 2) if bit == 0 else 3 - v


def exchange_kernel(
    samples, marks_ref, counts_ref, series_ref, theirs_ref, map_ref, target_ref, live_at,
    sk_out, ends_out, sums_out, meta_out, live_out,
    x_buf, own, ends_nat, ends_slots, sums_nat, sums_slots, meta_v, live_v, idx_v, idx_ref, lbuf, lgot,
    in_sem, idx_sem, d2d_send, d2d_recv, cube_send, cube_recv, st_send, st_recv, l_send, l_recv, loc_sem,
    *rest, step,
):
    acc, prt, out, outs, got, gots = (rest[PARTS * i : PARTS * (i + 1)] for i in range(6))
    steps = BLK // step
    parts = tuple(range(PARTS))

    def in_copy(i):
        part = pl.ds(i * step, step)
        return pltpu.make_async_copy(samples.at[part], x_buf.at[part], in_sem.at[i])

    for i in range(steps):
        in_copy(i).start()

    shard = lax.axis_index("shard")
    y = lax.axis_index("replica")
    core = lax.rem(shard, 2)
    x = lax.rem(lax.div(shard, 2), 4)
    z = lax.div(shard, 8)

    def across(dims):
        v = {"x": x, "y": y, "z": z}
        for d in dims:
            axis, bit = DIMS[d]
            v[axis] = flip(v[axis], bit)
        return {"shard": v["z"] * 8 + v["x"] * 2 + core, "replica": v["y"]}

    def bit_of(d):
        axis, bit = DIMS[d]
        v = {"x": x, "y": y, "z": z}[axis]
        high = lax.div(v, 2)
        return high if bit == 1 else lax.rem(v + high, 2)

    bits = [bit_of(d) for d in range(6)]
    partner = {"shard": shard + 1 - 2 * core, "replica": y}

    barrier = pltpu.get_barrier_semaphore()

    def greet(d, _):
        pl.semaphore_signal(barrier, inc=1, device_id={"shard": lax.rem(shard + d, SHARDS), "replica": y})
        return 0

    lax.fori_loop(1, SHARDS, greet, 0)
    for dims in OFF_PLANE:
        pl.semaphore_signal(barrier, inc=1, device_id=across(dims))

    map_row = map_ref[...]
    pos, owner, rank, pos_r, owner_r = routing(series_ref[...], map_row)
    sub, lane = iota((BLK, BLK), 0), iota((BLK, BLK), 1)
    before = jnp.max(jnp.where((pos == pos_r) & (sub < lane), sub, -1), axis=0, keepdims=True)
    idx_v[0:1, 0:BLK] = jnp.where(before < 0, BLK, jnp.minimum(before, BLK))
    idx_v[1:2, 0:BLK] = counts_ref[...]
    block = iota((BLK, LANES), 0)
    filled = iota((BLK, LANES), 1) == owner * CAP + rank
    idx_v[2:3, :] = jnp.clip(jnp.max(jnp.where(filled, block, 0), axis=0, keepdims=True), 0, BLK - 1)
    their_pos = routing(theirs_ref[...], map_row)[0]
    for p in parts:
        want = target_ref[p : p + 1, :] + core * 8
        for k, at in enumerate((pos, their_pos)):
            hit = jnp.max(jnp.where(at == want, block, -1), axis=0, keepdims=True)
            row = 8 + k * PARTS + p
            idx_v[row : row + 1, :] = jnp.where(hit < 0, BLK, jnp.minimum(hit, BLK))
    idx_copy = pltpu.make_async_copy(idx_v, idx_ref, idx_sem)
    idx_copy.start()
    counts_row = counts_ref[...].astype(jnp.float32)
    counts_col = jnp.sum(jnp.where(sub == lane, counts_row, 0.0), axis=1, keepdims=True)
    for r in range(2):
        at = live_at[r : r + 1, :]
        live_v[r] = jnp.sum(jnp.where(pos == at, counts_col, 0.0), axis=0, keepdims=True)
    pick = jnp.where(iota((SHARDS, BLK), 0) == owner_r, 1.0, 0.0)
    put = jnp.where(iota((BLK, LANES), 1) == rank, counts_col, 0.0)
    meta = jnp.dot(pick, put, precision=lax.Precision.HIGHEST, preferred_element_type=jnp.float32)
    for o in range(SHARDS):
        meta_v[o] = meta[o : o + 1, :]
    own[BLK] = jnp.zeros((BINS, LANES), jnp.float32)
    for p in parts:
        prt[p][BLK] = jnp.zeros((ROWS, LANES), jnp.float32)
    idx_copy.wait()

    row_at = lax.broadcasted_iota(jnp.int32, (1, SAMPLES), 1)
    bins = lax.broadcasted_iota(jnp.int32, (BINS, SAMPLES), 0)
    first_row = lax.broadcasted_iota(jnp.int32, (16, SAMPLES), 0) * 60

    first_minute = lax.broadcasted_iota(jnp.int32, (8, LANES), 0) * 60

    def chunk(i, _):
        in_copy(i).wait()
        for j in range(step):
            b = i * step + j
            before, count = idx_ref[0, b], idx_ref[1, b]
            block = x_buf[b]
            live = row_at < count
            marks = jnp.where(live, marks_ref[pl.ds(b, 1), :], -1)
            hot = jnp.where(bins == marks, 1.0, 0.0).astype(jnp.bfloat16)
            at = jnp.where(live, row_at, -1)
            minute = jnp.where((at >= first_row) & (at < first_row + 60), 1.0, 0.0).astype(jnp.bfloat16)
            both = jnp.dot(jnp.concatenate([hot, minute], axis=0), block, preferred_element_type=jnp.float32)
            own[b] = own[before] + both[:BINS]
            rows = jnp.clip(count - first_minute, 1, 60).astype(jnp.float32)
            code = (both[BINS : BINS + 8] * ((LEVELS / LIMIT) / rows) + 32768.5).astype(jnp.int32)
            sums_nat[b] = (code[:4] << 16) | code[4:]
        return 0

    lax.fori_loop(0, steps, chunk, 0)
    pl.semaphore_wait(barrier, SHARDS - 1 + len(OFF_PLANE))

    def d2d(p):
        return pltpu.make_async_remote_copy(
            own.at[pl.ds(0, BLK), pl.ds(p * ROWS, ROWS)], prt[p].at[pl.ds(0, BLK)],
            d2d_send.at[p], d2d_recv.at[p], device_id=partner,
        )

    for p in parts:
        d2d(p).start()

    def live_copy(s, src, device):
        return pltpu.make_async_remote_copy(src, lgot.at[s], l_send.at[s], l_recv.at[s], device_id=device)

    live_copies = [live_copy(0, live_v.at[1 - core], partner)]
    live_copies[0].start()

    def ends(i, _):
        for j in range(4):
            b = i * 4 + j
            least, most = minute_extremes(x_buf[b], idx_ref[1, b])
            ends_nat[b] = jnp.concatenate([least, most], axis=0)
        return 0

    def st_copies(d, to, slot):
        device = {"shard": to, "replica": y}
        pairs = ((ends_slots, ends_out), (sums_slots, sums_out), (meta_v, meta_out))
        return [
            pltpu.make_async_remote_copy(
                src.at[to], dst.at[slot], st_send.at[k, d], st_recv.at[k, d], device_id=device
            )
            for k, (src, dst) in enumerate(pairs)
        ]

    kept = [
        pltpu.make_async_copy(src.at[shard], dst.at[shard], loc_sem.at[k])
        for k, (src, dst) in enumerate(((ends_slots, ends_out), (sums_slots, sums_out), (meta_v, meta_out)))
    ]

    def send_all_stats():
        def place(o, _):
            for c in range(CAP):
                b = idx_ref[2, o * CAP + c]
                ends_slots[o, c] = ends_nat[b]
                sums_slots[o, c] = sums_nat[b]
            return 0

        lax.fori_loop(0, SHARDS, place, 0)

        def send_stats(d, _):
            for c in st_copies(d, lax.rem(shard + d, SHARDS), shard):
                c.start()
            return 0

        lax.fori_loop(1, SHARDS, send_stats, 0)
        for c in kept:
            c.start()

    bases = {(p, k): [k * 64] for p in parts for k in range(2)}
    copies = {}

    def encode(v):
        size = jnp.max(jnp.abs(v), axis=0, keepdims=True)
        gain = jnp.where(size > TINY, LEVELS / jnp.maximum(size, TINY), 0.0)
        code = (v * gain + 32768.5).astype(jnp.int32)
        return (code[:8] << 16) | code[8:], size

    def decode(word, size):
        unit = size * (1.0 / LEVELS)
        high = lax.shift_right_logical(word, 16).astype(jnp.float32)
        low = (word & 0xFFFF).astype(jnp.float32)
        return jnp.concatenate([(high - 32768.0) * unit, (low - 32768.0) * unit], axis=0)

    def each(n, fn):
        unroll = min(n, 8)

        def body(i, _):
            for u in range(unroll):
                fn(i * unroll + u)
            return 0

        lax.fori_loop(0, n // unroll, body, 0)

    def densify(p, lo, to=None):
        rows = pl.ds(p * ROWS, ROWS)

        def one(i):
            e = lo + i
            v = own[idx_ref[8 + p, e], rows] + prt[p][idx_ref[8 + PARTS + p, e]]
            if to is None:
                acc[p][e] = v
            else:
                out[p][to + i], outs[p][to + i] = encode(v)

        each(32, one)

    def add_in(p, at, lo, n, to=None):
        def one(i):
            v = acc[p][at + i] + decode(got[p][lo + i], gots[p][lo + i])
            if to is None:
                acc[p][at + i] = v
            else:
                out[p][to + i], outs[p][to + i] = encode(v)

        each(n, one)

    def spot(k, s):
        return k * 56 + 64 - (64 >> s)

    def send(p, slot, lo, n, device):
        region = pl.ds(lo, n)
        both = [
            pltpu.make_async_remote_copy(
                src[p].at[region], dst[p].at[region], cube_send.at[j, p, slot], cube_recv.at[j, p, slot], device_id=device,
            )
            for j, (src, dst) in enumerate(((out, got), (outs, gots)))
        ]
        for c in both:
            c.start()
        copies[p, slot] = both

    def halve(p, k, s):
        d = GROUPS[p][k][s]
        half = 32 >> s
        send(p, k * HALVINGS + s, spot(k, s), half, across((d,)))
        bases[p, k].append(bases[p, k][s] + bits[d] * half)

    for p in parts:
        lax.fori_loop(p * 2, p * 2 + 2, ends, 0)
        d2d(p).wait_recv()
        for k in range(2):
            bit = bits[GROUPS[p][k][0]]
            densify(p, k * 64 + (1 - bit) * 32, spot(k, 0))
            halve(p, k, 0)
            densify(p, k * 64 + bit * 32)
    send_all_stats()

    live_copies[0].wait_recv()
    lbuf[0] = live_v[core] + lgot[0]

    def live_step(s):
        live_copies.append(live_copy(s, lbuf.at[s - 1], across((GROUPS[0][0][s - 1],))))
        live_copies[s].start()

    live_step(1)
    ready = set()
    for p, k, s in EVENTS:
        if (p, k) == (0, 0):
            live_copies[s].wait_recv()
            lbuf[s] = lbuf[s - 1] + lgot[s]
            if s < HALVINGS:
                live_step(s + 1)
            else:
                for m, dims in enumerate(last_groups(0), 1):
                    c = live_copy(HALVINGS + m, lbuf.at[HALVINGS], across(dims))
                    c.start()
                    live_copies.append(c)
        for c in copies[p, k * HALVINGS + s - 1]:
            c.wait_recv()
        base, lo, half = bases[p, k][s], spot(k, s - 1), 32 >> (s - 1)
        if s < HALVINGS:
            quarter = half // 2
            bit = bits[GROUPS[p][k][s]]
            away = (1 - bit) * quarter
            add_in(p, base + away, lo + away, quarter, spot(k, s))
            halve(p, k, s)
            add_in(p, base + bit * quarter, lo + bit * quarter, quarter)
            continue
        add_in(p, base, lo, half)
        ready.add((p, k))
        if (p, 1 - k) not in ready:
            continue
        for m, dims in enumerate(last_groups(p), 1):
            theirs = 0
            for w, d in zip((4, 2, 1), TAILS[p]):
                theirs = theirs + (1 - bits[d] if d in dims else bits[d]) * w
            at = 112 + (m - 1) * 2
            for j in range(2):
                out[p][at + j], outs[p][at + j] = encode(acc[p][bases[p, j][HALVINGS] + theirs])
            send(p, 2 * HALVINGS + m - 1, at, 2, across(dims))
    for p in parts:
        mine = bits[TAILS[p][0]] * 4 + bits[TAILS[p][1]] * 2 + bits[TAILS[p][2]]
        v = [acc[p][bases[p, k][HALVINGS] + mine] for k in range(2)]
        for m in range(1, 8):
            for c in copies[p, 2 * HALVINGS + m - 1]:
                c.wait_recv()
            at = 112 + (m - 1) * 2
            v = [v[k] + decode(got[p][at + k], gots[p][at + k]) for k in range(2)]
        for k in range(2):
            sk_out[k, p * ROWS : (p + 1) * ROWS, :] = v[k]
    total = lbuf[HALVINGS]
    for m in range(1, 8):
        live_copies[HALVINGS + m].wait_recv()
        total = total + lgot[HALVINGS + m]
    live_out[...] = total

    def wait_stats(d, _):
        for c in st_copies(d, shard, lax.rem(shard - d + SHARDS, SHARDS)):
            c.wait_recv()
        return 0

    lax.fori_loop(1, SHARDS, wait_stats, 0)

    def wait_sends(d, _):
        for c in st_copies(d, lax.rem(shard + d, SHARDS), shard):
            c.wait_send()
        return 0

    lax.fori_loop(1, SHARDS, wait_sends, 0)
    for c in kept:
        c.wait()
    for c in live_copies:
        c.wait_send()
    for p in parts:
        d2d(p).wait_send()
    for both in copies.values():
        for c in both:
            c.wait_send()


def exchange_call(samples, marks, counts, series, theirs, owner_map):
    step = 8
    vmem = pl.BlockSpec(memory_space=pltpu.VMEM)
    any_ = pl.BlockSpec(memory_space=pl.ANY)
    lane = np.arange(LANES)
    live_at = np.stack([(lane // 8) * 16 + r * 8 + lane % 8 for r in (0, 1)]).astype(np.int32)
    i32, f32, bf16 = jnp.int32, jnp.float32, jnp.bfloat16
    dma = pltpu.SemaphoreType.DMA
    scratch = [
        pltpu.VMEM((BLK, SAMPLES, LANES), bf16),
        pltpu.VMEM((BLK + 1, BINS, LANES), f32),
        pltpu.VMEM((BLK, 16, LANES), bf16),
        pltpu.VMEM((SHARDS, CAP, 16, LANES), bf16),
        pltpu.VMEM((BLK, 4, LANES), i32),
        pltpu.VMEM((SHARDS, CAP, 4, LANES), i32),
        pltpu.VMEM((SHARDS, 1, LANES), f32),
        pltpu.VMEM((2, 1, LANES), f32),
        pltpu.VMEM((8 + 2 * PARTS, 128), i32),
        pltpu.SMEM((8 + 2 * PARTS, 128), i32),
        pltpu.VMEM((HALVINGS + 1, 1, LANES), f32),
        pltpu.VMEM((HALVINGS + 8, 1, LANES), f32),
        dma((BLK // step,)),
        dma,
        dma((PARTS,)),
        dma((PARTS,)),
        dma((2, PARTS, 2 * HALVINGS + 7)),
        dma((2, PARTS, 2 * HALVINGS + 7)),
        dma((3, SHARDS)),
        dma((3, SHARDS)),
        dma((HALVINGS + 8,)),
        dma((HALVINGS + 8,)),
        dma((3,)),
    ]
    scratch += [pltpu.VMEM((128, ROWS, LANES), f32)] * PARTS + [pltpu.VMEM((BLK + 1, ROWS, LANES), f32)] * PARTS
    scratch += ([pltpu.VMEM((126, 8, LANES), i32)] * PARTS + [pltpu.VMEM((126, 1, LANES), f32)] * PARTS) * 2
    return pl.pallas_call(
        functools.partial(exchange_kernel, step=step),
        in_specs=[any_] + [vmem] * 7,
        out_specs=[vmem, any_, any_, any_, vmem],
        out_shape=[
            jax.ShapeDtypeStruct((2, BINS, LANES), f32),
            jax.ShapeDtypeStruct((SHARDS, CAP, 16, LANES), bf16),
            jax.ShapeDtypeStruct((SHARDS, CAP, 4, LANES), i32),
            jax.ShapeDtypeStruct((SHARDS, 1, LANES), f32),
            jax.ShapeDtypeStruct((1, LANES), f32),
        ],
        scratch_shapes=scratch,
        compiler_params=pltpu.CompilerParams(
            collective_id=0, has_side_effects=True, vmem_limit_bytes=60 * 2**20
        ),
        name="exchange",
    )(
        samples, marks, counts.reshape(1, BLK), series.reshape(1, BLK), theirs.reshape(1, BLK),
        owner_map.reshape(1, -1), jnp.asarray(part_positions()), jnp.asarray(live_at),
    )


def finish_kernel(
    meta, ends, sums, sk_in, live_in, cold, sk_out, live_out,
    counts, ends_buf, sums_buf, cold_buf, sk_buf, live_buf, in_sem, out_sem, one_sem, *, step,
):
    steps = SHARDS // step

    def loads(i):
        part = pl.ds(i * step, step)
        return [
            pltpu.make_async_copy(src.at[part], dst.at[part], in_sem.at[k, i])
            for k, (src, dst) in enumerate(((ends, ends_buf), (sums, sums_buf)))
        ]

    def store(i):
        part = pl.ds(i * step * CAP, step * CAP)
        return pltpu.make_async_copy(cold_buf.at[part], cold.at[part], out_sem.at[i])

    singles = [
        pltpu.make_async_copy(src, dst, one_sem.at[k])
        for k, (src, dst) in enumerate(((meta, counts), (sk_in, sk_buf), (live_in, live_buf), (sk_buf, sk_out)))
    ]
    singles[0].start()
    for i in range(steps):
        for c in loads(i):
            c.start()
    singles[1].start()
    singles[2].start()
    minute = lax.broadcasted_iota(jnp.int32, (8, LANES), 0).astype(jnp.float32) * 60.0
    singles[0].wait()
    for i in range(steps):
        for c in loads(i):
            c.wait()

        def group(g, _):
            source = i * step + g
            for c in range(CAP):
                at = source * CAP + c
                count = jnp.clip(counts[source, 0, c] - minute, 0.0, 60.0)
                filled = count > 0
                low_high = ends_buf[source, c].astype(jnp.float32)
                word = sums_buf[source, c]
                code = jnp.concatenate([lax.shift_right_logical(word, 16), word & 0xFFFF], axis=0)
                total = (code.astype(jnp.float32) - 32768.0) * (count * (LIMIT / LEVELS))
                cold_buf[at, 0] = jnp.where(filled, low_high[0:8], 0.0)
                cold_buf[at, 1] = jnp.where(filled, low_high[8:16], 0.0)
                cold_buf[at, 2] = jnp.where(filled, total, 0.0)
                cold_buf[at, 3] = count
            return 0

        lax.fori_loop(0, step, group, 0)
        store(i).start()
    singles[1].wait()
    singles[3].start()
    singles[2].wait()
    place = lax.div(lax.axis_index("shard"), 2) * 8 + lax.axis_index("replica") * 2
    lane = lax.broadcasted_iota(jnp.int32, (1, LANES), 1)
    for k in range(2):
        live_out[k] = jnp.sum(jnp.where(lane == place + k, live_buf[...], 0.0))
    singles[3].wait()
    for i in range(steps):
        store(i).wait()


def finish_call(meta, ends, sums, sketches, live):
    step = 8
    smem = pl.BlockSpec(memory_space=pltpu.SMEM)
    any_ = pl.BlockSpec(memory_space=pl.ANY)
    f32 = jnp.float32
    return pl.pallas_call(
        functools.partial(finish_kernel, step=step),
        in_specs=[any_] * 5,
        out_specs=[any_, any_, smem],
        out_shape=[
            jax.ShapeDtypeStruct((SHARDS * CAP, 4, 8, LANES), f32),
            jax.ShapeDtypeStruct((2, BINS, LANES), f32),
            jax.ShapeDtypeStruct((2,), f32),
        ],
        scratch_shapes=[
            pltpu.SMEM((SHARDS, 1, LANES), f32),
            pltpu.VMEM((SHARDS, CAP, 16, LANES), jnp.bfloat16),
            pltpu.VMEM((SHARDS, CAP, 4, LANES), jnp.int32),
            pltpu.VMEM((SHARDS * CAP, 4, 8, LANES), f32),
            pltpu.VMEM((2, BINS, LANES), f32),
            pltpu.VMEM((1, LANES), f32),
            pltpu.SemaphoreType.DMA((2, SHARDS // step)),
            pltpu.SemaphoreType.DMA((SHARDS // step,)),
            pltpu.SemaphoreType.DMA((4,)),
        ],
        name="finish",
    )(meta, ends, sums, sketches, live)


def body(samples, counts, buckets, block_series, owner_map):
    swap = [(i, i ^ 1) for i in range(SHARDS)]
    theirs = lax.ppermute(block_series, "shard", swap)
    sk, ends, sums, meta, live = exchange_call(samples, buckets, counts, block_series, theirs, owner_map)
    cold, sketches, live_rows = finish_call(meta, ends, sums, sk, live)
    return cold.reshape(1, 1, SHARDS * CAP, 4, 8, LANES), sketches, live_rows


def solution(mesh):
    return jax.shard_map(
        body,
        mesh=mesh,
        in_specs=(
            P(("shard", "replica"), None, None),
            P(("shard", "replica")),
            P(("shard", "replica"), None),
            P(("shard", "replica")),
            P(),
        ),
        out_specs=(
            P("shard", "replica", None, None, None, None),
            P(("shard", "replica"), None, None),
            P(("shard", "replica")),
        ),
        check_vma=False,
    )
```

```python
import functools

import jax
import jax.numpy as jnp
import numpy as np
from jax import lax
from jax.experimental import pallas as pl
from jax.experimental.pallas import tpu as pltpu
from jax.sharding import PartitionSpec as P

BINS = 128
LANES = 128
SAMPLES = 480
BLK = 64
SHARDS = 32
REPLICAS = 4
CAP = 4
DIMS = (("x", 0), ("z", 0), ("y", 0), ("x", 1), ("z", 1), ("y", 1))
GROUPS = (((4, 5, 1), (1, 5, 4)), ((5, 2, 3), (2, 5, 3)), ((3, 2, 5), (5, 3, 2)), ((2, 4, 0), (4, 0, 2)), ((0, 2, 5), (0, 5, 2)), ((5, 1, 2), (2, 5, 1)), ((1, 3, 2), (3, 2, 1)), ((2, 5, 4), (4, 5, 2)))
EVENTS = ((0, 0, 1), (0, 1, 1), (1, 0, 1), (1, 1, 1), (2, 0, 1), (4, 0, 1), (3, 1, 1), (2, 1, 1), (3, 0, 1), (6, 0, 1), (6, 1, 1), (4, 1, 1), (7, 1, 1), (5, 0, 1), (5, 1, 1), (0, 0, 2), (2, 1, 2), (3, 1, 2), (0, 1, 2), (7, 0, 1), (6, 0, 2), (3, 0, 2), (5, 0, 2), (1, 1, 2), (1, 0, 2), (4, 1, 2), (0, 0, 3), (2, 0, 2), (7, 1, 2), (4, 0, 2), (5, 1, 2), (6, 1, 2), (0, 1, 3), (3, 0, 3), (2, 1, 3), (7, 0, 2), (1, 1, 3), (3, 1, 3), (2, 0, 3), (6, 0, 3), (1, 0, 3), (4, 0, 3), (5, 0, 3), (5, 1, 3), (4, 1, 3), (6, 1, 3), (7, 1, 3), (7, 0, 3))
TAILS = tuple(tuple(d for d in range(6) if d not in g[0]) for g in GROUPS)
PARTS = len(GROUPS)
ROWS = BINS // PARTS
LIMIT = 6.0
LEVELS = 32766.0
TINY = 1e-33
GRAY = {(0, 0): 0, (0, 1): 1, (1, 1): 2, (1, 0): 3}


HALVINGS = 3


def last_groups(p):
    return [tuple(d for k, d in enumerate(TAILS[p]) if m >> k & 1) for m in range(1, 8)]


def off_plane():
    dims = {(d,) for g in GROUPS for d in g[0]}
    dims |= {tuple(sorted(g)) for p in range(PARTS) for g in last_groups(p)}
    return tuple(sorted(g for g in dims if any(DIMS[d][0] == "y" for d in g)))


OFF_PLANE = off_plane()
STATS_ORDER = tuple(sorted(range(1, SHARDS), key=lambda d: (-min((d // 8) % 4, 4 - (d // 8) % 4), -min((d // 2) % 4, 4 - (d // 2) % 4), d)))


def part_positions():
    table = np.zeros((PARTS, 128), np.int32)
    for p in range(PARTS):
        for k in range(2):
            order = GROUPS[p][k] + TAILS[p]
            for i in range(64):
                bits = {DIMS[d]: (i >> (5 - s)) & 1 for s, d in enumerate(order)}
                x, y, z = (GRAY[(bits[(a, 1)], bits[(a, 0)])] for a in "xyz")
                table[p, k * 64 + i] = (z * 4 + x) * 16 + y * 2 + k
    return table


def minute_extremes(x, count):
    sub16 = lax.broadcasted_iota(jnp.int16, (16, LANES), 0)
    sub = lax.broadcasted_iota(jnp.int32, (8, LANES), 0)
    least = jnp.zeros((8, LANES), jnp.float32)
    most = jnp.zeros((8, LANES), jnp.float32)
    inf = jnp.bfloat16(jnp.inf)
    for q in range(2):
        lo = [None] * 4
        hi = [None] * 4
        for v in range(15):
            at_row = 240 * q + 16 * v
            val = x[at_row : at_row + 16]
            ok = sub16 < jnp.full((16, LANES), jnp.clip(count - at_row, 0, 16), jnp.int32).astype(jnp.int16)
            small, large = jnp.where(ok, val, inf), jnp.where(ok, val, -inf)
            for h in range(4):
                a, b = 60 * h - 16 * v, 60 * h + 60 - 16 * v
                if b <= 0 or a >= 16:
                    continue
                s, g = small, large
                if a > 0:
                    s, g = jnp.where(sub16 >= a, s, inf), jnp.where(sub16 >= a, g, -inf)
                if b < 16:
                    s, g = jnp.where(sub16 < b, s, inf), jnp.where(sub16 < b, g, -inf)
                lo[h] = s if lo[h] is None else jnp.minimum(lo[h], s)
                hi[h] = g if hi[h] is None else jnp.maximum(hi[h], g)
        for h in range(4):
            m = 4 * q + h
            least = jnp.where(sub == m, jnp.min(lo[h].astype(jnp.float32), axis=0, keepdims=True), least)
            most = jnp.where(sub == m, jnp.max(hi[h].astype(jnp.float32), axis=0, keepdims=True), most)
    return least.astype(jnp.bfloat16), most.astype(jnp.bfloat16)


def iota(shape, dim):
    return lax.broadcasted_iota(jnp.int32, shape, dim)


def routing(series_row, map_row):
    sub, lane = iota((BLK, BLK), 0), iota((BLK, BLK), 1)
    eye = sub == lane

    def row(col):
        return jnp.sum(jnp.where(eye, col, 0), axis=0, keepdims=True)

    series = jnp.sum(jnp.where(eye, series_row, 0), axis=1, keepdims=True)
    pos = jnp.sum(jnp.where(iota((BLK, 256), 1) == series, map_row, 0), axis=1, keepdims=True)
    pos_r = row(pos)
    owner, owner_r = pos >> 3, pos_r >> 3
    rank = jnp.sum(jnp.where((owner == owner_r) & (lane < sub), 1, 0), axis=1, keepdims=True)
    return pos, owner, rank, pos_r, owner_r


def flip(v, bit):
    return v + 1 - 2 * lax.rem(v, 2) if bit == 0 else 3 - v


def exchange_kernel(
    samples, marks_ref, counts_ref, series_ref, map_ref, target_ref, live_at,
    sk_out, ends_out, sums_out, meta_out, live_out,
    x_buf, own, ends_nat, ends_slots, sums_nat, sums_slots, meta_v, live_v, idx_v, idx_ref, their_series, their_v, their_idx, lbuf, lgot,
    in_sem, idx_sem, series_sem, d2d_send, d2d_recv, cube_send, cube_recv, st_send, st_recv, l_send, l_recv, loc_sem,
    *rest, step,
):
    acc, prt, out, outs, got, gots = (rest[PARTS * i : PARTS * (i + 1)] for i in range(6))
    steps = BLK // step
    parts = tuple(range(PARTS))

    def in_copy(i):
        part = pl.ds(i * step, step)
        return pltpu.make_async_copy(samples.at[part], x_buf.at[part], in_sem.at[i])

    for i in range(steps):
        in_copy(i).start()

    shard = lax.axis_index("shard")
    y = lax.axis_index("replica")
    core = lax.rem(shard, 2)
    x = lax.rem(lax.div(shard, 2), 4)
    z = lax.div(shard, 8)

    def across(dims):
        v = {"x": x, "y": y, "z": z}
        for d in dims:
            axis, bit = DIMS[d]
            v[axis] = flip(v[axis], bit)
        return {"shard": v["z"] * 8 + v["x"] * 2 + core, "replica": v["y"]}

    def bit_of(d):
        axis, bit = DIMS[d]
        v = {"x": x, "y": y, "z": z}[axis]
        high = lax.div(v, 2)
        return high if bit == 1 else lax.rem(v + high, 2)

    bits = [bit_of(d) for d in range(6)]
    partner = {"shard": shard + 1 - 2 * core, "replica": y}

    barrier = pltpu.get_barrier_semaphore()

    def greet(d, _):
        pl.semaphore_signal(barrier, inc=1, device_id={"shard": lax.rem(shard + d, SHARDS), "replica": y})
        return 0

    lax.fori_loop(1, SHARDS, greet, 0)
    for dims in OFF_PLANE:
        pl.semaphore_signal(barrier, inc=1, device_id=across(dims))

    map_row = map_ref[...]
    pos, owner, rank, pos_r, owner_r = routing(series_ref[...], map_row)
    sub, lane = iota((BLK, BLK), 0), iota((BLK, BLK), 1)
    before = jnp.max(jnp.where((pos == pos_r) & (sub < lane), sub, -1), axis=0, keepdims=True)
    idx_v[0:1, 0:BLK] = jnp.where(before < 0, BLK, jnp.minimum(before, BLK))
    idx_v[1:2, 0:BLK] = counts_ref[...]
    block = iota((BLK, LANES), 0)
    filled = iota((BLK, LANES), 1) == owner * CAP + rank
    idx_v[2:3, :] = jnp.clip(jnp.max(jnp.where(filled, block, 0), axis=0, keepdims=True), 0, BLK - 1)

    def last_blocks(at, to, first):
        for p in parts:
            hit = jnp.max(jnp.where(at == target_ref[p : p + 1, :] + core * 8, block, -1), axis=0, keepdims=True)
            to[first + p : first + p + 1, :] = jnp.where(hit < 0, BLK, jnp.minimum(hit, BLK))

    last_blocks(pos, idx_v, 8)
    idx_copy = pltpu.make_async_copy(idx_v, idx_ref, idx_sem.at[0])
    idx_copy.start()
    counts_row = counts_ref[...].astype(jnp.float32)
    counts_col = jnp.sum(jnp.where(sub == lane, counts_row, 0.0), axis=1, keepdims=True)
    for r in range(2):
        at = live_at[r : r + 1, :]
        live_v[r] = jnp.sum(jnp.where(pos == at, counts_col, 0.0), axis=0, keepdims=True)
    pick = jnp.where(iota((SHARDS, BLK), 0) == owner_r, 1.0, 0.0)
    put = jnp.where(iota((BLK, LANES), 1) == rank, counts_col, 0.0)
    meta = jnp.dot(pick, put, precision=lax.Precision.HIGHEST, preferred_element_type=jnp.float32)
    for o in range(SHARDS):
        meta_v[o] = meta[o : o + 1, :]
    own[BLK] = jnp.zeros((BINS, LANES), jnp.float32)
    for p in parts:
        prt[p][BLK] = jnp.zeros((ROWS, LANES), jnp.float32)
    idx_copy.wait()

    row_at = lax.broadcasted_iota(jnp.int32, (1, SAMPLES), 1)
    bins = lax.broadcasted_iota(jnp.int32, (BINS, SAMPLES), 0)
    first_row = lax.broadcasted_iota(jnp.int32, (16, SAMPLES), 0) * 60

    first_minute = lax.broadcasted_iota(jnp.int32, (8, LANES), 0) * 60

    def chunk(i, _):
        in_copy(i).wait()
        for j in range(step):
            b = i * step + j
            before, count = idx_ref[0, b], idx_ref[1, b]
            block = x_buf[b]
            live = row_at < count
            marks = jnp.where(live, marks_ref[pl.ds(b, 1), :], -1)
            hot = jnp.where(bins == marks, 1.0, 0.0).astype(jnp.bfloat16)
            at = jnp.where(live, row_at, -1)
            minute = jnp.where((at >= first_row) & (at < first_row + 60), 1.0, 0.0).astype(jnp.bfloat16)
            both = jnp.dot(jnp.concatenate([hot, minute], axis=0), block, preferred_element_type=jnp.float32)
            own[b] = own[before] + both[:BINS]
            rows = jnp.clip(count - first_minute, 1, 60).astype(jnp.float32)
            code = (both[BINS : BINS + 8] * ((LEVELS / LIMIT) / rows) + 32768.5).astype(jnp.int32)
            sums_nat[b] = (code[:4] << 16) | code[4:]
        return 0

    lax.fori_loop(0, steps, chunk, 0)
    pl.semaphore_wait(barrier, SHARDS - 1 + len(OFF_PLANE))

    def d2d(p):
        return pltpu.make_async_remote_copy(
            own.at[pl.ds(0, BLK), pl.ds(p * ROWS, ROWS)], prt[p].at[pl.ds(0, BLK)],
            d2d_send.at[p], d2d_recv.at[p], device_id=partner,
        )

    series_copy = pltpu.make_async_remote_copy(
        series_ref, their_series, series_sem.at[0], series_sem.at[1], device_id=partner
    )
    series_copy.start()
    for p in parts[:4]:
        d2d(p).start()

    def live_copy(s, src, device):
        return pltpu.make_async_remote_copy(src, lgot.at[s], l_send.at[s], l_recv.at[s], device_id=device)

    live_copies = [live_copy(0, live_v.at[1 - core], partner)]
    live_copies[0].start()

    def ends(i, _):
        for j in range(4):
            b = i * 4 + j
            least, most = minute_extremes(x_buf[b], idx_ref[1, b])
            ends_nat[b] = jnp.concatenate([least, most], axis=0)
        return 0

    def st_copies(d, to, slot):
        device = {"shard": to, "replica": y}
        pairs = ((ends_slots, ends_out), (sums_slots, sums_out), (meta_v, meta_out))
        return [
            pltpu.make_async_remote_copy(
                src.at[to], dst.at[slot], st_send.at[k, d], st_recv.at[k, d], device_id=device
            )
            for k, (src, dst) in enumerate(pairs)
        ]

    kept = [
        pltpu.make_async_copy(src.at[shard], dst.at[shard], loc_sem.at[k])
        for k, (src, dst) in enumerate(((ends_slots, ends_out), (sums_slots, sums_out), (meta_v, meta_out)))
    ]

    def place(o, _):
        for c in range(CAP):
            b = idx_ref[2, o * CAP + c]
            ends_slots[o, c] = ends_nat[b]
            sums_slots[o, c] = sums_nat[b]
        return 0

    peers = iter(STATS_ORDER)

    def next_stats():
        d = next(peers, None)
        if d is not None:
            for c in st_copies(d, lax.rem(shard + d, SHARDS), shard):
                c.start()

    bases = {(p, k): [k * 64] for p in parts for k in range(2)}
    copies = {}

    def encode(v):
        size = jnp.max(jnp.abs(v), axis=0, keepdims=True)
        gain = jnp.where(size > TINY, LEVELS / jnp.maximum(size, TINY), 0.0)
        code = (v * gain + 32768.5).astype(jnp.int32)
        return (code[:8] << 16) | code[8:], size

    def decode(word, size):
        unit = size * (1.0 / LEVELS)
        high = lax.shift_right_logical(word, 16).astype(jnp.float32)
        low = (word & 0xFFFF).astype(jnp.float32)
        return jnp.concatenate([(high - 32768.0) * unit, (low - 32768.0) * unit], axis=0)

    def each(n, fn):
        unroll = min(n, 8)

        def body(i, _):
            for u in range(unroll):
                fn(i * unroll + u)
            return 0

        lax.fori_loop(0, n // unroll, body, 0)

    def densify(p, lo, to=None):
        rows = pl.ds(p * ROWS, ROWS)

        def one(i):
            e = lo + i
            v = own[idx_ref[8 + p, e], rows] + prt[p][their_idx[p, e]]
            if to is None:
                acc[p][e] = v
            else:
                out[p][to + i], outs[p][to + i] = encode(v)

        each(32, one)

    def add_in(p, at, lo, n, to=None):
        def one(i):
            v = acc[p][at + i] + decode(got[p][lo + i], gots[p][lo + i])
            if to is None:
                acc[p][at + i] = v
            else:
                out[p][to + i], outs[p][to + i] = encode(v)

        each(n, one)

    def spot(k, s):
        return k * 56 + 64 - (64 >> s)

    def send(p, slot, lo, n, device):
        region = pl.ds(lo, n)
        both = [
            pltpu.make_async_remote_copy(
                src[p].at[region], dst[p].at[region], cube_send.at[j, p, slot], cube_recv.at[j, p, slot], device_id=device,
            )
            for j, (src, dst) in enumerate(((out, got), (outs, gots)))
        ]
        for c in both:
            c.start()
        copies[p, slot] = both

    def halve(p, k, s):
        d = GROUPS[p][k][s]
        half = 32 >> s
        send(p, k * HALVINGS + s, spot(k, s), half, across((d,)))
        bases[p, k].append(bases[p, k][s] + bits[d] * half)

    lax.fori_loop(0, 3, ends, 0)
    series_copy.wait_recv()
    last_blocks(routing(their_series[...], map_row)[0], their_v, 0)
    their_copy = pltpu.make_async_copy(their_v, their_idx, idx_sem.at[1])
    their_copy.start()
    lax.fori_loop(3, 7, ends, 0)
    their_copy.wait()
    for p in parts:
        d2d(p).wait_recv()
        if p + 4 < PARTS:
            d2d(p + 4).start()
        for k in range(2):
            bit = bits[GROUPS[p][k][0]]
            densify(p, k * 64 + (1 - bit) * 32, spot(k, 0))
            halve(p, k, 0)
            densify(p, k * 64 + bit * 32)

    lax.fori_loop(7, BLK // 4, ends, 0)
    lax.fori_loop(0, SHARDS, place, 0)
    for c in kept:
        c.start()
    live_copies[0].wait_recv()
    lbuf[0] = live_v[core] + lgot[0]

    def live_step(s):
        live_copies.append(live_copy(s, lbuf.at[s - 1], across((GROUPS[0][0][s - 1],))))
        live_copies[s].start()

    live_step(1)
    ready = set()
    for p, k, s in EVENTS:
        if (p, k) == (0, 0):
            live_copies[s].wait_recv()
            lbuf[s] = lbuf[s - 1] + lgot[s]
            if s < HALVINGS:
                live_step(s + 1)
            else:
                for m, dims in enumerate(last_groups(0), 1):
                    c = live_copy(HALVINGS + m, lbuf.at[HALVINGS], across(dims))
                    c.start()
                    live_copies.append(c)
        for c in copies[p, k * HALVINGS + s - 1]:
            c.wait_recv()
        next_stats()
        base, lo, half = bases[p, k][s], spot(k, s - 1), 32 >> (s - 1)
        if s < HALVINGS:
            quarter = half // 2
            bit = bits[GROUPS[p][k][s]]
            away = (1 - bit) * quarter
            add_in(p, base + away, lo + away, quarter, spot(k, s))
            halve(p, k, s)
            add_in(p, base + bit * quarter, lo + bit * quarter, quarter)
            continue
        add_in(p, base, lo, half)
        ready.add((p, k))
        if (p, 1 - k) not in ready:
            continue
        values = []
        for dims in last_groups(p):
            theirs = 0
            for w, d in zip((4, 2, 1), TAILS[p]):
                theirs = theirs + (1 - bits[d] if d in dims else bits[d]) * w
            values += [acc[p][bases[p, j][HALVINGS] + theirs] for j in range(2)]
        for i, (word, size) in enumerate([encode(v) for v in values]):
            out[p][112 + i], outs[p][112 + i] = word, size
        for m, dims in enumerate(last_groups(p), 1):
            send(p, 2 * HALVINGS + m - 1, 112 + (m - 1) * 2, 2, across(dims))
    def wait_stats(d, _):
        for c in st_copies(d, shard, lax.rem(shard - d + SHARDS, SHARDS)):
            c.wait_recv()
        for c in st_copies(d, lax.rem(shard + d, SHARDS), shard):
            c.wait_send()
        return 0

    for p in parts:
        d2d(p).wait_send()
        for slot in range(2 * HALVINGS):
            for c in copies[p, slot]:
                c.wait_send()
    series_copy.wait_send()
    lax.fori_loop(1, SHARDS, wait_stats, 0)
    for c in kept:
        c.wait()

    for p in parts:
        mine = bits[TAILS[p][0]] * 4 + bits[TAILS[p][1]] * 2 + bits[TAILS[p][2]]
        v = [acc[p][bases[p, k][HALVINGS] + mine] for k in range(2)]
        for m in range(1, 8):
            for c in copies[p, 2 * HALVINGS + m - 1]:
                c.wait_recv()
            at = 112 + (m - 1) * 2
            v = [v[k] + decode(got[p][at + k], gots[p][at + k]) for k in range(2)]
        for k in range(2):
            sk_out[k, p * ROWS : (p + 1) * ROWS, :] = v[k]
    total = lbuf[HALVINGS]
    for m in range(1, 8):
        live_copies[HALVINGS + m].wait_recv()
        total = total + lgot[HALVINGS + m]
    live_out[...] = total

    for c in live_copies:
        c.wait_send()
    for p in parts:
        for slot in range(2 * HALVINGS, 2 * HALVINGS + 7):
            for c in copies[p, slot]:
                c.wait_send()


def exchange_call(samples, marks, counts, series, owner_map):
    step = 8
    vmem = pl.BlockSpec(memory_space=pltpu.VMEM)
    any_ = pl.BlockSpec(memory_space=pl.ANY)
    lane = np.arange(LANES)
    live_at = np.stack([(lane // 8) * 16 + r * 8 + lane % 8 for r in (0, 1)]).astype(np.int32)
    i32, f32, bf16 = jnp.int32, jnp.float32, jnp.bfloat16
    dma = pltpu.SemaphoreType.DMA
    scratch = [
        pltpu.VMEM((BLK, SAMPLES, LANES), bf16),
        pltpu.VMEM((BLK + 1, BINS, LANES), f32),
        pltpu.VMEM((BLK, 16, LANES), bf16),
        pltpu.VMEM((SHARDS, CAP, 16, LANES), bf16),
        pltpu.VMEM((BLK, 4, LANES), i32),
        pltpu.VMEM((SHARDS, CAP, 4, LANES), i32),
        pltpu.VMEM((SHARDS, 1, LANES), f32),
        pltpu.VMEM((2, 1, LANES), f32),
        pltpu.VMEM((8 + PARTS, 128), i32),
        pltpu.SMEM((8 + PARTS, 128), i32),
        pltpu.VMEM((1, BLK), i32),
        pltpu.VMEM((PARTS, 128), i32),
        pltpu.SMEM((PARTS, 128), i32),
        pltpu.VMEM((HALVINGS + 1, 1, LANES), f32),
        pltpu.VMEM((HALVINGS + 8, 1, LANES), f32),
        dma((BLK // step,)),
        dma((2,)),
        dma((2,)),
        dma((PARTS,)),
        dma((PARTS,)),
        dma((2, PARTS, 2 * HALVINGS + 7)),
        dma((2, PARTS, 2 * HALVINGS + 7)),
        dma((3, SHARDS)),
        dma((3, SHARDS)),
        dma((HALVINGS + 8,)),
        dma((HALVINGS + 8,)),
        dma((3,)),
    ]
    scratch += [pltpu.VMEM((128, ROWS, LANES), f32)] * PARTS + [pltpu.VMEM((BLK + 1, ROWS, LANES), f32)] * PARTS
    scratch += ([pltpu.VMEM((126, 8, LANES), i32)] * PARTS + [pltpu.VMEM((126, 1, LANES), f32)] * PARTS) * 2
    return pl.pallas_call(
        functools.partial(exchange_kernel, step=step),
        in_specs=[any_] + [vmem] * 6,
        out_specs=[vmem, any_, any_, any_, vmem],
        out_shape=[
            jax.ShapeDtypeStruct((2, BINS, LANES), f32),
            jax.ShapeDtypeStruct((SHARDS, CAP, 16, LANES), bf16),
            jax.ShapeDtypeStruct((SHARDS, CAP, 4, LANES), i32),
            jax.ShapeDtypeStruct((SHARDS, 1, LANES), f32),
            jax.ShapeDtypeStruct((1, LANES), f32),
        ],
        scratch_shapes=scratch,
        compiler_params=pltpu.CompilerParams(
            collective_id=0, has_side_effects=True, vmem_limit_bytes=60 * 2**20
        ),
        name="exchange",
    )(
        samples, marks, counts.reshape(1, BLK), series.reshape(1, BLK), owner_map.reshape(1, -1),
        jnp.asarray(part_positions()), jnp.asarray(live_at),
    )


def finish_kernel(
    meta, ends, sums, sk_in, live_in, cold, sk_out, live_out,
    counts, ends_buf, sums_buf, cold_buf, sk_buf, live_buf, in_sem, out_sem, one_sem, *, step,
):
    steps = SHARDS // step

    def loads(i):
        part = pl.ds(i * step, step)
        return [
            pltpu.make_async_copy(src.at[part], dst.at[part], in_sem.at[k, i])
            for k, (src, dst) in enumerate(((ends, ends_buf), (sums, sums_buf)))
        ]

    def store(i):
        part = pl.ds(i * step * CAP, step * CAP)
        return pltpu.make_async_copy(cold_buf.at[part], cold.at[part], out_sem.at[i])

    singles = [
        pltpu.make_async_copy(src, dst, one_sem.at[k])
        for k, (src, dst) in enumerate(((meta, counts), (sk_in, sk_buf), (live_in, live_buf), (sk_buf, sk_out)))
    ]
    singles[0].start()
    for i in range(steps):
        for c in loads(i):
            c.start()
    singles[1].start()
    singles[2].start()
    minute = lax.broadcasted_iota(jnp.int32, (8, LANES), 0).astype(jnp.float32) * 60.0
    singles[0].wait()
    for i in range(steps):
        for c in loads(i):
            c.wait()

        def group(g, _):
            source = i * step + g
            for c in range(CAP):
                at = source * CAP + c
                count = jnp.clip(counts[source, 0, c] - minute, 0.0, 60.0)
                filled = count > 0
                low_high = ends_buf[source, c].astype(jnp.float32)
                word = sums_buf[source, c]
                code = jnp.concatenate([lax.shift_right_logical(word, 16), word & 0xFFFF], axis=0)
                total = (code.astype(jnp.float32) - 32768.0) * (count * (LIMIT / LEVELS))
                cold_buf[at, 0] = jnp.where(filled, low_high[0:8], 0.0)
                cold_buf[at, 1] = jnp.where(filled, low_high[8:16], 0.0)
                cold_buf[at, 2] = jnp.where(filled, total, 0.0)
                cold_buf[at, 3] = count
            return 0

        lax.fori_loop(0, step, group, 0)
        store(i).start()
    singles[1].wait()
    singles[3].start()
    singles[2].wait()
    place = lax.div(lax.axis_index("shard"), 2) * 8 + lax.axis_index("replica") * 2
    lane = lax.broadcasted_iota(jnp.int32, (1, LANES), 1)
    for k in range(2):
        live_out[k] = jnp.sum(jnp.where(lane == place + k, live_buf[...], 0.0))
    singles[3].wait()
    for i in range(steps):
        store(i).wait()


def finish_call(meta, ends, sums, sketches, live):
    step = 8
    smem = pl.BlockSpec(memory_space=pltpu.SMEM)
    any_ = pl.BlockSpec(memory_space=pl.ANY)
    f32 = jnp.float32
    return pl.pallas_call(
        functools.partial(finish_kernel, step=step),
        in_specs=[any_] * 5,
        out_specs=[any_, any_, smem],
        out_shape=[
            jax.ShapeDtypeStruct((SHARDS * CAP, 4, 8, LANES), f32),
            jax.ShapeDtypeStruct((2, BINS, LANES), f32),
            jax.ShapeDtypeStruct((2,), f32),
        ],
        scratch_shapes=[
            pltpu.SMEM((SHARDS, 1, LANES), f32),
            pltpu.VMEM((SHARDS, CAP, 16, LANES), jnp.bfloat16),
            pltpu.VMEM((SHARDS, CAP, 4, LANES), jnp.int32),
            pltpu.VMEM((SHARDS * CAP, 4, 8, LANES), f32),
            pltpu.VMEM((2, BINS, LANES), f32),
            pltpu.VMEM((1, LANES), f32),
            pltpu.SemaphoreType.DMA((2, SHARDS // step)),
            pltpu.SemaphoreType.DMA((SHARDS // step,)),
            pltpu.SemaphoreType.DMA((4,)),
        ],
        name="finish",
    )(meta, ends, sums, sketches, live)


def body(samples, counts, buckets, block_series, owner_map):
    sk, ends, sums, meta, live = exchange_call(samples, buckets, counts, block_series, owner_map)
    cold, sketches, live_rows = finish_call(meta, ends, sums, sk, live)
    return cold.reshape(1, 1, SHARDS * CAP, 4, 8, LANES), sketches, live_rows


def solution(mesh):
    return jax.shard_map(
        body,
        mesh=mesh,
        in_specs=(
            P(("shard", "replica"), None, None),
            P(("shard", "replica")),
            P(("shard", "replica"), None),
            P(("shard", "replica")),
            P(),
        ),
        out_specs=(
            P("shard", "replica", None, None, None, None),
            P(("shard", "replica"), None, None),
            P(("shard", "replica")),
        ),
        check_vma=False,
    )
```

```python
import functools

import jax
import jax.numpy as jnp
import numpy as np
from jax import lax
from jax.experimental import pallas as pl
from jax.experimental.pallas import tpu as pltpu
from jax.sharding import PartitionSpec as P

BINS = 128
LANES = 128
SAMPLES = 480
BLK = 64
SHARDS = 32
REPLICAS = 4
CAP = 4
DIMS = (("x", 0), ("z", 0), ("y", 0), ("x", 1), ("z", 1), ("y", 1))
GROUPS = (((4, 5, 1), (1, 5, 4)), ((5, 2, 3), (2, 5, 3)), ((3, 2, 5), (5, 3, 2)), ((2, 4, 0), (4, 0, 2)), ((0, 2, 5), (0, 5, 2)), ((5, 1, 2), (2, 5, 1)), ((1, 3, 2), (3, 2, 1)), ((2, 5, 4), (4, 5, 2)))
EVENTS = ((0, 0, 1), (0, 1, 1), (1, 0, 1), (1, 1, 1), (2, 0, 1), (4, 0, 1), (3, 1, 1), (2, 1, 1), (3, 0, 1), (6, 0, 1), (6, 1, 1), (4, 1, 1), (7, 1, 1), (5, 0, 1), (5, 1, 1), (0, 0, 2), (2, 1, 2), (3, 1, 2), (0, 1, 2), (7, 0, 1), (6, 0, 2), (3, 0, 2), (5, 0, 2), (1, 1, 2), (1, 0, 2), (4, 1, 2), (0, 0, 3), (2, 0, 2), (7, 1, 2), (4, 0, 2), (5, 1, 2), (6, 1, 2), (0, 1, 3), (3, 0, 3), (2, 1, 3), (7, 0, 2), (1, 1, 3), (3, 1, 3), (2, 0, 3), (6, 0, 3), (1, 0, 3), (4, 0, 3), (5, 0, 3), (5, 1, 3), (4, 1, 3), (6, 1, 3), (7, 1, 3), (7, 0, 3))
TAILS = tuple(tuple(d for d in range(6) if d not in g[0]) for g in GROUPS)
PARTS = len(GROUPS)
READY = tuple(sorted(range(PARTS), key=lambda p: max(i for i, e in enumerate(EVENTS) if e[0] == p)))
ROWS = BINS // PARTS
LIMIT = 6.0
LEVELS = 32766.0
TINY = 1e-33
GRAY = {(0, 0): 0, (0, 1): 1, (1, 1): 2, (1, 0): 3}


HALVINGS = 3


def last_groups(p):
    return [tuple(d for k, d in enumerate(TAILS[p]) if m >> k & 1) for m in range(1, 8)]


def off_plane():
    dims = {(d,) for g in GROUPS for d in g[0]}
    dims |= {tuple(sorted(g)) for p in range(PARTS) for g in last_groups(p)}
    return tuple(sorted(g for g in dims if any(DIMS[d][0] == "y" for d in g)))


OFF_PLANE = off_plane()
STATS_ORDER = tuple(sorted(range(1, SHARDS), key=lambda d: (-min((d // 8) % 4, 4 - (d // 8) % 4), -min((d // 2) % 4, 4 - (d // 2) % 4), d)))


def part_positions():
    table = np.zeros((PARTS, 128), np.int32)
    for p in range(PARTS):
        for k in range(2):
            order = GROUPS[p][k] + TAILS[p]
            for i in range(64):
                bits = {DIMS[d]: (i >> (5 - s)) & 1 for s, d in enumerate(order)}
                x, y, z = (GRAY[(bits[(a, 1)], bits[(a, 0)])] for a in "xyz")
                table[p, k * 64 + i] = (z * 4 + x) * 16 + y * 2 + k
    return table


def minute_extremes(x, count):
    sub16 = lax.broadcasted_iota(jnp.int16, (16, LANES), 0)
    sub = lax.broadcasted_iota(jnp.int32, (8, LANES), 0)
    least = jnp.zeros((8, LANES), jnp.float32)
    most = jnp.zeros((8, LANES), jnp.float32)
    inf = jnp.bfloat16(jnp.inf)
    for q in range(2):
        lo = [None] * 4
        hi = [None] * 4
        for v in range(15):
            at_row = 240 * q + 16 * v
            val = x[at_row : at_row + 16]
            ok = sub16 < jnp.full((16, LANES), jnp.clip(count - at_row, 0, 16), jnp.int32).astype(jnp.int16)
            small, large = jnp.where(ok, val, inf), jnp.where(ok, val, -inf)
            for h in range(4):
                a, b = 60 * h - 16 * v, 60 * h + 60 - 16 * v
                if b <= 0 or a >= 16:
                    continue
                s, g = small, large
                if a > 0:
                    s, g = jnp.where(sub16 >= a, s, inf), jnp.where(sub16 >= a, g, -inf)
                if b < 16:
                    s, g = jnp.where(sub16 < b, s, inf), jnp.where(sub16 < b, g, -inf)
                lo[h] = s if lo[h] is None else jnp.minimum(lo[h], s)
                hi[h] = g if hi[h] is None else jnp.maximum(hi[h], g)
        for h in range(4):
            m = 4 * q + h
            least = jnp.where(sub == m, jnp.min(lo[h].astype(jnp.float32), axis=0, keepdims=True), least)
            most = jnp.where(sub == m, jnp.max(hi[h].astype(jnp.float32), axis=0, keepdims=True), most)
    return least.astype(jnp.bfloat16), most.astype(jnp.bfloat16)


def iota(shape, dim):
    return lax.broadcasted_iota(jnp.int32, shape, dim)


def routing(series_row, map_row):
    sub, lane = iota((BLK, BLK), 0), iota((BLK, BLK), 1)
    eye = sub == lane

    def row(col):
        return jnp.sum(jnp.where(eye, col, 0), axis=0, keepdims=True)

    series = jnp.sum(jnp.where(eye, series_row, 0), axis=1, keepdims=True)
    pos = jnp.sum(jnp.where(iota((BLK, 256), 1) == series, map_row, 0), axis=1, keepdims=True)
    pos_r = row(pos)
    owner, owner_r = pos >> 3, pos_r >> 3
    rank = jnp.sum(jnp.where((owner == owner_r) & (lane < sub), 1, 0), axis=1, keepdims=True)
    return pos, owner, rank, pos_r, owner_r


def flip(v, bit):
    return v + 1 - 2 * lax.rem(v, 2) if bit == 0 else 3 - v


def exchange_kernel(
    samples, marks_ref, counts_ref, series_ref, map_ref, target_ref, live_at,
    sk_out, ends_out, sums_out, meta_out, live_out,
    x_buf, own, ends_nat, ends_slots, sums_nat, sums_slots, meta_v, live_v, idx_v, idx_ref, their_series, their_v, their_idx, lbuf, lgot,
    in_sem, idx_sem, series_sem, d2d_send, d2d_recv, cube_send, cube_recv, st_send, st_recv, l_send, l_recv, loc_sem,
    *rest, step,
):
    acc, prt, out, outs, got, gots = (rest[PARTS * i : PARTS * (i + 1)] for i in range(6))
    steps = BLK // step
    parts = tuple(range(PARTS))

    def in_copy(i):
        part = pl.ds(i * step, step)
        return pltpu.make_async_copy(samples.at[part], x_buf.at[part], in_sem.at[i])

    for i in range(steps):
        in_copy(i).start()

    shard = lax.axis_index("shard")
    y = lax.axis_index("replica")
    core = lax.rem(shard, 2)
    x = lax.rem(lax.div(shard, 2), 4)
    z = lax.div(shard, 8)

    def across(dims):
        v = {"x": x, "y": y, "z": z}
        for d in dims:
            axis, bit = DIMS[d]
            v[axis] = flip(v[axis], bit)
        return {"shard": v["z"] * 8 + v["x"] * 2 + core, "replica": v["y"]}

    def bit_of(d):
        axis, bit = DIMS[d]
        v = {"x": x, "y": y, "z": z}[axis]
        high = lax.div(v, 2)
        return high if bit == 1 else lax.rem(v + high, 2)

    bits = [bit_of(d) for d in range(6)]
    partner = {"shard": shard + 1 - 2 * core, "replica": y}

    barrier = pltpu.get_barrier_semaphore()

    def greet(d, _):
        pl.semaphore_signal(barrier, inc=1, device_id={"shard": lax.rem(shard + d, SHARDS), "replica": y})
        return 0

    lax.fori_loop(1, SHARDS, greet, 0)
    for dims in OFF_PLANE:
        pl.semaphore_signal(barrier, inc=1, device_id=across(dims))

    map_row = map_ref[...]
    pos, owner, rank, pos_r, owner_r = routing(series_ref[...], map_row)
    sub, lane = iota((BLK, BLK), 0), iota((BLK, BLK), 1)
    before = jnp.max(jnp.where((pos == pos_r) & (sub < lane), sub, -1), axis=0, keepdims=True)
    idx_v[0:1, 0:BLK] = jnp.where(before < 0, BLK, jnp.minimum(before, BLK))
    idx_v[1:2, 0:BLK] = counts_ref[...]
    block = iota((BLK, LANES), 0)
    filled = iota((BLK, LANES), 1) == owner * CAP + rank
    idx_v[2:3, :] = jnp.clip(jnp.max(jnp.where(filled, block, 0), axis=0, keepdims=True), 0, BLK - 1)

    def last_blocks(at, to, first):
        for p in parts:
            hit = jnp.max(jnp.where(at == target_ref[p : p + 1, :] + core * 8, block, -1), axis=0, keepdims=True)
            to[first + p : first + p + 1, :] = jnp.where(hit < 0, BLK, jnp.minimum(hit, BLK))

    last_blocks(pos, idx_v, 8)
    idx_copy = pltpu.make_async_copy(idx_v, idx_ref, idx_sem.at[0])
    idx_copy.start()
    counts_row = counts_ref[...].astype(jnp.float32)
    counts_col = jnp.sum(jnp.where(sub == lane, counts_row, 0.0), axis=1, keepdims=True)
    for r in range(2):
        at = live_at[r : r + 1, :]
        live_v[r] = jnp.sum(jnp.where(pos == at, counts_col, 0.0), axis=0, keepdims=True)
    pick = jnp.where(iota((SHARDS, BLK), 0) == owner_r, 1.0, 0.0)
    put = jnp.where(iota((BLK, LANES), 1) == rank, counts_col, 0.0)
    meta = jnp.dot(pick, put, precision=lax.Precision.HIGHEST, preferred_element_type=jnp.float32)
    for o in range(SHARDS):
        meta_v[o] = meta[o : o + 1, :]
    own[BLK] = jnp.zeros((BINS, LANES), jnp.float32)
    for p in parts:
        prt[p][BLK] = jnp.zeros((ROWS, LANES), jnp.float32)
    idx_copy.wait()

    row_at = lax.broadcasted_iota(jnp.int32, (1, SAMPLES), 1)
    bins = lax.broadcasted_iota(jnp.int32, (BINS, SAMPLES), 0)
    first_row = lax.broadcasted_iota(jnp.int32, (16, SAMPLES), 0) * 60

    first_minute = lax.broadcasted_iota(jnp.int32, (8, LANES), 0) * 60

    def chunk(i, _):
        in_copy(i).wait()
        for j in range(step):
            b = i * step + j
            before, count = idx_ref[0, b], idx_ref[1, b]
            block = x_buf[b]
            live = row_at < count
            marks = jnp.where(live, marks_ref[pl.ds(b, 1), :], -1)
            hot = jnp.where(bins == marks, 1.0, 0.0).astype(jnp.bfloat16)
            at = jnp.where(live, row_at, -1)
            minute = jnp.where((at >= first_row) & (at < first_row + 60), 1.0, 0.0).astype(jnp.bfloat16)
            both = jnp.dot(jnp.concatenate([hot, minute], axis=0), block, preferred_element_type=jnp.float32)
            own[b] = own[before] + both[:BINS]
            rows = jnp.clip(count - first_minute, 1, 60).astype(jnp.float32)
            code = (both[BINS : BINS + 8] * ((LEVELS / LIMIT) / rows) + 32768.5).astype(jnp.int32)
            sums_nat[b] = (code[:4] << 16) | code[4:]
        return 0

    lax.fori_loop(0, steps, chunk, 0)
    pl.semaphore_wait(barrier, SHARDS - 1 + len(OFF_PLANE))

    def d2d(p):
        return pltpu.make_async_remote_copy(
            own.at[pl.ds(0, BLK), pl.ds(p * ROWS, ROWS)], prt[p].at[pl.ds(0, BLK)],
            d2d_send.at[p], d2d_recv.at[p], device_id=partner,
        )

    series_copy = pltpu.make_async_remote_copy(
        series_ref, their_series, series_sem.at[0], series_sem.at[1], device_id=partner
    )
    series_copy.start()
    for p in parts[:4]:
        d2d(p).start()

    def live_copy(s, src, device):
        return pltpu.make_async_remote_copy(src, lgot.at[s], l_send.at[s], l_recv.at[s], device_id=device)

    live_copies = [live_copy(0, live_v.at[1 - core], partner)]
    live_copies[0].start()

    def ends(i, _):
        for j in range(4):
            b = i * 4 + j
            least, most = minute_extremes(x_buf[b], idx_ref[1, b])
            ends_nat[b] = jnp.concatenate([least, most], axis=0)
        return 0

    def st_copies(d, to, slot):
        device = {"shard": to, "replica": y}
        pairs = ((ends_slots, ends_out), (sums_slots, sums_out), (meta_v, meta_out))
        return [
            pltpu.make_async_remote_copy(
                src.at[to], dst.at[slot], st_send.at[k, d], st_recv.at[k, d], device_id=device
            )
            for k, (src, dst) in enumerate(pairs)
        ]

    kept = [
        pltpu.make_async_copy(src.at[shard], dst.at[shard], loc_sem.at[k])
        for k, (src, dst) in enumerate(((ends_slots, ends_out), (sums_slots, sums_out), (meta_v, meta_out)))
    ]

    def place(o, _):
        for c in range(CAP):
            b = idx_ref[2, o * CAP + c]
            ends_slots[o, c] = ends_nat[b]
            sums_slots[o, c] = sums_nat[b]
        return 0

    peers = iter(STATS_ORDER)

    def next_stats():
        d = next(peers, None)
        if d is not None:
            for c in st_copies(d, lax.rem(shard + d, SHARDS), shard):
                c.start()

    bases = {(p, k): [k * 64] for p in parts for k in range(2)}
    copies = {}

    def encode(v):
        size = jnp.max(jnp.abs(v), axis=0, keepdims=True)
        gain = jnp.where(size > TINY, LEVELS / jnp.maximum(size, TINY), 0.0)
        code = (v * gain + 32768.5).astype(jnp.int32)
        return (code[:8] << 16) | code[8:], size

    def decode(word, size):
        unit = size * (1.0 / LEVELS)
        high = lax.shift_right_logical(word, 16).astype(jnp.float32)
        low = (word & 0xFFFF).astype(jnp.float32)
        return jnp.concatenate([(high - 32768.0) * unit, (low - 32768.0) * unit], axis=0)

    def each(n, fn):
        unroll = min(n, 8)

        def body(i, _):
            for u in range(unroll):
                fn(i * unroll + u)
            return 0

        lax.fori_loop(0, n // unroll, body, 0)

    def densify(p, lo, to=None):
        rows = pl.ds(p * ROWS, ROWS)

        def one(i):
            e = lo + i
            v = own[idx_ref[8 + p, e], rows] + prt[p][their_idx[p, e]]
            if to is None:
                acc[p][e] = v
            else:
                out[p][to + i], outs[p][to + i] = encode(v)

        each(32, one)

    def add_in(p, at, lo, n, to=None):
        def one(i):
            v = acc[p][at + i] + decode(got[p][lo + i], gots[p][lo + i])
            if to is None:
                acc[p][at + i] = v
            else:
                out[p][to + i], outs[p][to + i] = encode(v)

        each(n, one)

    def spot(k, s):
        return k * 56 + 64 - (64 >> s)

    def send(p, slot, lo, n, device):
        region = pl.ds(lo, n)
        both = [
            pltpu.make_async_remote_copy(
                src[p].at[region], dst[p].at[region], cube_send.at[j, p, slot], cube_recv.at[j, p, slot], device_id=device,
            )
            for j, (src, dst) in enumerate(((out, got), (outs, gots)))
        ]
        for c in both:
            c.start()
        copies[p, slot] = both

    def halve(p, k, s):
        d = GROUPS[p][k][s]
        half = 32 >> s
        send(p, k * HALVINGS + s, spot(k, s), half, across((d,)))
        bases[p, k].append(bases[p, k][s] + bits[d] * half)

    lax.fori_loop(0, 2, ends, 0)
    series_copy.wait_recv()
    last_blocks(routing(their_series[...], map_row)[0], their_v, 0)
    their_copy = pltpu.make_async_copy(their_v, their_idx, idx_sem.at[1])
    their_copy.start()
    lax.fori_loop(2, 3, ends, 0)
    their_copy.wait()
    for p in parts:
        d2d(p).wait_recv()
        if p + 4 < PARTS:
            d2d(p + 4).start()
        for k in range(2):
            bit = bits[GROUPS[p][k][0]]
            densify(p, k * 64 + (1 - bit) * 32, spot(k, 0))
            halve(p, k, 0)
            densify(p, k * 64 + bit * 32)

    lax.fori_loop(3, BLK // 4, ends, 0)
    lax.fori_loop(0, SHARDS, place, 0)
    for c in kept:
        c.start()
    live_copies[0].wait_recv()
    lbuf[0] = live_v[core] + lgot[0]

    def live_step(s):
        live_copies.append(live_copy(s, lbuf.at[s - 1], across((GROUPS[0][0][s - 1],))))
        live_copies[s].start()

    live_step(1)
    ready = set()
    for p, k, s in EVENTS:
        if (p, k) == (0, 0):
            live_copies[s].wait_recv()
            lbuf[s] = lbuf[s - 1] + lgot[s]
            if s < HALVINGS:
                live_step(s + 1)
            else:
                for m, dims in enumerate(last_groups(0), 1):
                    c = live_copy(HALVINGS + m, lbuf.at[HALVINGS], across(dims))
                    c.start()
                    live_copies.append(c)
        for c in copies[p, k * HALVINGS + s - 1]:
            c.wait_recv()
        next_stats()
        base, lo, half = bases[p, k][s], spot(k, s - 1), 32 >> (s - 1)
        if s < HALVINGS:
            quarter = half // 2
            bit = bits[GROUPS[p][k][s]]
            away = (1 - bit) * quarter
            add_in(p, base + away, lo + away, quarter, spot(k, s))
            halve(p, k, s)
            add_in(p, base + bit * quarter, lo + bit * quarter, quarter)
            continue
        add_in(p, base, lo, half)
        ready.add((p, k))
        if (p, 1 - k) not in ready:
            continue
        values = []
        for dims in last_groups(p):
            theirs = 0
            for w, d in zip((4, 2, 1), TAILS[p]):
                theirs = theirs + (1 - bits[d] if d in dims else bits[d]) * w
            values += [acc[p][bases[p, j][HALVINGS] + theirs] for j in range(2)]
        for i, (word, size) in enumerate([encode(v) for v in values]):
            out[p][112 + i], outs[p][112 + i] = word, size
        for m, dims in enumerate(last_groups(p), 1):
            send(p, 2 * HALVINGS + m - 1, 112 + (m - 1) * 2, 2, across(dims))
    def wait_stats(d, _):
        for c in st_copies(d, shard, lax.rem(shard - d + SHARDS, SHARDS)):
            c.wait_recv()
        for c in st_copies(d, lax.rem(shard + d, SHARDS), shard):
            c.wait_send()
        return 0

    for p in parts:
        d2d(p).wait_send()
        for slot in range(2 * HALVINGS):
            for c in copies[p, slot]:
                c.wait_send()
    series_copy.wait_send()
    lax.fori_loop(1, SHARDS, wait_stats, 0)
    for c in kept:
        c.wait()

    for p in READY:
        mine = bits[TAILS[p][0]] * 4 + bits[TAILS[p][1]] * 2 + bits[TAILS[p][2]]
        v = [acc[p][bases[p, k][HALVINGS] + mine] for k in range(2)]
        for m in range(1, 8):
            for c in copies[p, 2 * HALVINGS + m - 1]:
                c.wait_recv()
            at = 112 + (m - 1) * 2
            v = [v[k] + decode(got[p][at + k], gots[p][at + k]) for k in range(2)]
        for k in range(2):
            sk_out[k, p * ROWS : (p + 1) * ROWS, :] = v[k]
    total = lbuf[HALVINGS]
    for m in range(1, 8):
        live_copies[HALVINGS + m].wait_recv()
        total = total + lgot[HALVINGS + m]
    live_out[...] = total

    for c in live_copies:
        c.wait_send()
    for p in parts:
        for slot in range(2 * HALVINGS, 2 * HALVINGS + 7):
            for c in copies[p, slot]:
                c.wait_send()


def exchange_call(samples, marks, counts, series, owner_map):
    step = 8
    vmem = pl.BlockSpec(memory_space=pltpu.VMEM)
    any_ = pl.BlockSpec(memory_space=pl.ANY)
    lane = np.arange(LANES)
    live_at = np.stack([(lane // 8) * 16 + r * 8 + lane % 8 for r in (0, 1)]).astype(np.int32)
    i32, f32, bf16 = jnp.int32, jnp.float32, jnp.bfloat16
    dma = pltpu.SemaphoreType.DMA
    scratch = [
        pltpu.VMEM((BLK, SAMPLES, LANES), bf16),
        pltpu.VMEM((BLK + 1, BINS, LANES), f32),
        pltpu.VMEM((BLK, 16, LANES), bf16),
        pltpu.VMEM((SHARDS, CAP, 16, LANES), bf16),
        pltpu.VMEM((BLK, 4, LANES), i32),
        pltpu.VMEM((SHARDS, CAP, 4, LANES), i32),
        pltpu.VMEM((SHARDS, 1, LANES), f32),
        pltpu.VMEM((2, 1, LANES), f32),
        pltpu.VMEM((8 + PARTS, 128), i32),
        pltpu.SMEM((8 + PARTS, 128), i32),
        pltpu.VMEM((1, BLK), i32),
        pltpu.VMEM((PARTS, 128), i32),
        pltpu.SMEM((PARTS, 128), i32),
        pltpu.VMEM((HALVINGS + 1, 1, LANES), f32),
        pltpu.VMEM((HALVINGS + 8, 1, LANES), f32),
        dma((BLK // step,)),
        dma((2,)),
        dma((2,)),
        dma((PARTS,)),
        dma((PARTS,)),
        dma((2, PARTS, 2 * HALVINGS + 7)),
        dma((2, PARTS, 2 * HALVINGS + 7)),
        dma((3, SHARDS)),
        dma((3, SHARDS)),
        dma((HALVINGS + 8,)),
        dma((HALVINGS + 8,)),
        dma((3,)),
    ]
    scratch += [pltpu.VMEM((128, ROWS, LANES), f32)] * PARTS + [pltpu.VMEM((BLK + 1, ROWS, LANES), f32)] * PARTS
    scratch += ([pltpu.VMEM((126, 8, LANES), i32)] * PARTS + [pltpu.VMEM((126, 1, LANES), f32)] * PARTS) * 2
    return pl.pallas_call(
        functools.partial(exchange_kernel, step=step),
        in_specs=[any_] + [vmem] * 6,
        out_specs=[vmem, any_, any_, any_, vmem],
        out_shape=[
            jax.ShapeDtypeStruct((2, BINS, LANES), f32),
            jax.ShapeDtypeStruct((SHARDS, CAP, 16, LANES), bf16),
            jax.ShapeDtypeStruct((SHARDS, CAP, 4, LANES), i32),
            jax.ShapeDtypeStruct((SHARDS, 1, LANES), f32),
            jax.ShapeDtypeStruct((1, LANES), f32),
        ],
        scratch_shapes=scratch,
        compiler_params=pltpu.CompilerParams(
            collective_id=0, has_side_effects=True, vmem_limit_bytes=60 * 2**20
        ),
        name="exchange",
    )(
        samples, marks, counts.reshape(1, BLK), series.reshape(1, BLK), owner_map.reshape(1, -1),
        jnp.asarray(part_positions()), jnp.asarray(live_at),
    )


def finish_kernel(
    meta, ends, sums, sk_in, live_in, cold, sk_out, live_out,
    counts, ends_buf, sums_buf, cold_buf, sk_buf, live_buf, in_sem, out_sem, one_sem, *, step,
):
    steps = SHARDS // step

    def loads(i):
        part = pl.ds(i * step, step)
        return [
            pltpu.make_async_copy(src.at[part], dst.at[part], in_sem.at[k, i])
            for k, (src, dst) in enumerate(((ends, ends_buf), (sums, sums_buf)))
        ]

    def store(i):
        part = pl.ds(i * step * CAP, step * CAP)
        return pltpu.make_async_copy(cold_buf.at[part], cold.at[part], out_sem.at[i])

    singles = [
        pltpu.make_async_copy(src, dst, one_sem.at[k])
        for k, (src, dst) in enumerate(((meta, counts), (sk_in, sk_buf), (live_in, live_buf), (sk_buf, sk_out)))
    ]
    singles[0].start()
    for i in range(steps):
        for c in loads(i):
            c.start()
    singles[1].start()
    singles[2].start()
    minute = lax.broadcasted_iota(jnp.int32, (8, LANES), 0).astype(jnp.float32) * 60.0
    singles[0].wait()
    for i in range(steps):
        for c in loads(i):
            c.wait()

        def group(g, _):
            source = i * step + g
            for c in range(CAP):
                at = source * CAP + c
                count = jnp.clip(counts[source, 0, c] - minute, 0.0, 60.0)
                filled = count > 0
                low_high = ends_buf[source, c].astype(jnp.float32)
                word = sums_buf[source, c]
                code = jnp.concatenate([lax.shift_right_logical(word, 16), word & 0xFFFF], axis=0)
                total = (code.astype(jnp.float32) - 32768.0) * (count * (LIMIT / LEVELS))
                cold_buf[at, 0] = jnp.where(filled, low_high[0:8], 0.0)
                cold_buf[at, 1] = jnp.where(filled, low_high[8:16], 0.0)
                cold_buf[at, 2] = jnp.where(filled, total, 0.0)
                cold_buf[at, 3] = count
            return 0

        lax.fori_loop(0, step, group, 0)
        store(i).start()
    singles[1].wait()
    singles[3].start()
    singles[2].wait()
    place = lax.div(lax.axis_index("shard"), 2) * 8 + lax.axis_index("replica") * 2
    lane = lax.broadcasted_iota(jnp.int32, (1, LANES), 1)
    for k in range(2):
        live_out[k] = jnp.sum(jnp.where(lane == place + k, live_buf[...], 0.0))
    singles[3].wait()
    for i in range(steps):
        store(i).wait()


def finish_call(meta, ends, sums, sketches, live):
    step = 8
    smem = pl.BlockSpec(memory_space=pltpu.SMEM)
    any_ = pl.BlockSpec(memory_space=pl.ANY)
    f32 = jnp.float32
    return pl.pallas_call(
        functools.partial(finish_kernel, step=step),
        in_specs=[any_] * 5,
        out_specs=[any_, any_, smem],
        out_shape=[
            jax.ShapeDtypeStruct((SHARDS * CAP, 4, 8, LANES), f32),
            jax.ShapeDtypeStruct((2, BINS, LANES), f32),
            jax.ShapeDtypeStruct((2,), f32),
        ],
        scratch_shapes=[
            pltpu.SMEM((SHARDS, 1, LANES), f32),
            pltpu.VMEM((SHARDS, CAP, 16, LANES), jnp.bfloat16),
            pltpu.VMEM((SHARDS, CAP, 4, LANES), jnp.int32),
            pltpu.VMEM((SHARDS * CAP, 4, 8, LANES), f32),
            pltpu.VMEM((2, BINS, LANES), f32),
            pltpu.VMEM((1, LANES), f32),
            pltpu.SemaphoreType.DMA((2, SHARDS // step)),
            pltpu.SemaphoreType.DMA((SHARDS // step,)),
            pltpu.SemaphoreType.DMA((4,)),
        ],
        name="finish",
    )(meta, ends, sums, sketches, live)


def body(samples, counts, buckets, block_series, owner_map):
    sk, ends, sums, meta, live = exchange_call(samples, buckets, counts, block_series, owner_map)
    cold, sketches, live_rows = finish_call(meta, ends, sums, sk, live)
    return cold.reshape(1, 1, SHARDS * CAP, 4, 8, LANES), sketches, live_rows


def solution(mesh):
    return jax.shard_map(
        body,
        mesh=mesh,
        in_specs=(
            P(("shard", "replica"), None, None),
            P(("shard", "replica")),
            P(("shard", "replica"), None),
            P(("shard", "replica")),
            P(),
        ),
        out_specs=(
            P("shard", "replica", None, None, None, None),
            P(("shard", "replica"), None, None),
            P(("shard", "replica")),
        ),
        check_vma=False,
    )
```
